32 devices in a mesh: gx: 4 (over y, core), gy: 8 (over z, x).
Axes of the slice: x: 2, y: 2, z: 4, core: 2. Of those that a mesh axis runs over, the one named last changes fastest.
Arguments:
- old_master: float32 [32, 128, 1536], P('gx', 'gy'), may hold values from -3 to 3
- old_first: float32 [32, 128, 1536], P('gx', 'gy'), may hold values from -3 to 3
- old_second: float32 [32, 128, 1536], P('gx', 'gy'), may hold values from 0.01 to 1
- new_grad: bfloat16 [32, 128, 1536], P(('gx', 'gy')), may hold values from -3072 to 3072
- counts: int32 [32, 32], P(None, ('gx', 'gy')), may hold values from 1 to 72, as said below
- old_owner: int32 [32], replicated, may hold values from 0 to 31, each once
- new_owner: int32 [32], replicated, may hold values from 0 to 31, each once
Outputs:
- new_master: float32 [32, 128, 1536], P(('gx', 'gy'))
- new_first: float32 [32, 128, 1536], P(('gx', 'gy'))
- new_second: float32 [32, 128, 1536], P(('gx', 'gy'))
The draws below stay inside these ranges and needn't reach their ends.
Inputs may be any that keep to these rules, and one draw needn't show every extreme that they name: `old_owner`: every number of 0 to 31 appears once. `new_owner`: every number of 0 to 31 appears once. `counts`: every device routed at least one token to every expert.
All inputs are finite; a program needn't handle non-finite values.
Results may differ from the reference program's by a relative error of at most 0.0003.
Values sent between devices are 32-bit elements; how exact they have to be, the bound alone decides.
A program may use at most 64 MiB of HBM per device.

```python
import math
import jax
import jax.numpy as jnp
from jax import lax

FF = 1536
ROWS = 128
EXPERTS = 32
RANKS = 32


def draw_counts(key, part):
    key_tokens = jax.random.fold_in(key, 11)
    key_skew = jax.random.fold_in(key, 23)
    columns = jnp.arange(RANKS, dtype=jnp.int32)
    ceiling = 6 + 12 * columns // max(RANKS - 1, 1)
    factor = 1 + jax.random.randint(key_skew, (EXPERTS,), 0, 4)
    base = 1 + jax.random.randint(key_tokens, (EXPERTS, RANKS), 0, ceiling[None, :])
    return (base * factor[:, None]).astype(jnp.int32)


def block_scale(stream_key, dims, pieces, low, top_value):
    def one(axis_at, parts):
        heights = jax.random.uniform(jax.random.fold_in(jax.random.fold_in(stream_key, 6), axis_at), (parts,), jnp.float32, low / len(pieces), top_value / len(pieces))
        return jnp.repeat(jnp.exp(heights), dims[axis_at] // parts).reshape((-1,) + (1,) * (len(dims) - axis_at - 1))

    level = one(*pieces[0])
    for cut in pieces[1:]:
        level = level * one(*cut)
    return level


def bell_draw(key, extent, scale, limit, cuts=(), kind=jnp.bfloat16):
    values = jax.random.normal(key, extent, jnp.float32) * scale
    if len(cuts) > 0:
        values = block_scale(key, extent, cuts, -0.22, 0.18) * values
    return jnp.clip(values, min=-limit, max=limit).astype(kind)


def setup_inputs(seed: int = 0) -> dict:
    seeds = jax.random.split(jax.random.key(seed), 8)
    old_master = bell_draw(seeds[0], (EXPERTS, ROWS, FF), 0.5, 3.0, ((0, 4), (1, 8)), jnp.float32)
    old_first = bell_draw(seeds[1], (EXPERTS, ROWS, FF), 0.5, 3.0, ((0, 4), (1, 8)), jnp.float32)
    old_second = jnp.clip(jnp.exp(math.log(1.0) - 4.6051702 * jax.random.uniform(seeds[2], (EXPERTS, ROWS, FF), jnp.float32) ** block_scale(seeds[2], (EXPERTS, ROWS, FF), ((0, 4), (1, 8)), -0.2, 0.2)), 0.01, 1.0)
    new_grad = bell_draw(seeds[3], (EXPERTS, ROWS, FF), (16 * EXPERTS), 3072.0, ((0, 32),))
    counts = draw_counts(jax.random.fold_in(seeds[7], 71), 0)
    old_owner = jax.random.permutation(seeds[5], EXPERTS).astype(jnp.int32)
    new_owner = jax.random.permutation(seeds[6], EXPERTS).astype(jnp.int32)
    return {"old_master": old_master, "old_first": old_first, "old_second": old_second, "new_grad": new_grad, "counts": counts, "old_owner": old_owner, "new_owner": new_owner}


first_correction = 1.0 - 0.9 ** 10
second_correction = 1.0 - 0.999 ** 10

def adam_step(master, first, second, grad, slot_count):
    scaled = grad.astype(jnp.float32) / slot_count
    new_first = 0.9 * first + 0.1 * scaled
    new_second = 0.999 * second + 0.001 * scaled * scaled
    step_dir = new_first / first_correction / (jnp.sqrt(new_second / second_correction) + 1e-08)
    new_master = master - 0.01 * (step_dir + 0.1 * master)
    return (new_master, new_first, new_second)

def reference(old_master, old_first, old_second, new_grad, counts, old_owner, new_owner):
    slots = jnp.arange(EXPERTS, dtype=jnp.int32)
    onehot = new_owner[:, None] == slots[None, :]
    source = lax.optimization_barrier(jnp.sum(jnp.where(onehot, old_owner[:, None], 0), axis=0)).astype(jnp.int32)
    totals = lax.optimization_barrier(jnp.sum(counts.astype(jnp.float32), axis=1))
    slot_count = lax.optimization_barrier(jnp.sum(jnp.where(onehot, totals[:, None], jnp.float32(0.0)), axis=0))
    master = jnp.take(old_master, source, axis=0)
    first = jnp.take(old_first, source, axis=0)
    second = jnp.take(old_second, source, axis=0)
    return adam_step(master, first, second, new_grad, slot_count[:, None, None])
```

```python
import functools

import jax
import jax.numpy as jnp
from jax import lax
from jax.experimental import pallas as pl
from jax.experimental.pallas import tpu as pltpu
from jax.sharding import PartitionSpec as P

first_correction = 1.0 - 0.9**10
second_correction = 1.0 - 0.999**10
MESH = pl.DeviceIdType.MESH
LANES = 128
VMEM_GRANT = 24 << 20
SUBLANES = 8
PAIR = 2
STATES = 3
ADAM_ROWS = 16
PUBLISHED = 4
HOLD_LOW = 0
HOLD_HIGH = 0
BAND = 2
WIDTHS = (1, 2, 3)


def adam_step(master, first, second, grad, slot_count):
    scaled = grad.astype(jnp.float32) / slot_count
    new_first = 0.9 * first + 0.1 * scaled
    new_second = 0.999 * second + 0.001 * scaled * scaled
    step_dir = new_first / first_correction / (jnp.sqrt(new_second / second_correction) + 1e-08)
    new_master = master - 0.01 * (step_dir + 0.1 * master)
    return (new_master, new_first, new_second)


def adam_scaled(master, first, second, grad, per_token):
    scaled = grad.astype(jnp.float32) * per_token
    new_first = 0.9 * first + 0.1 * scaled
    new_second = 0.999 * second + 0.001 * scaled * scaled
    step_dir = new_first * (1.0 / first_correction) / (jnp.sqrt(new_second * (1.0 / second_correction)) + 1e-08)
    new_master = master - 0.01 * (step_dir + 0.1 * master)
    return (new_master, new_first, new_second)


def reorder(block, groups_x, groups_y):
    total_rows = block.shape[1]
    piece = total_rows // (groups_x * groups_y)
    shaped = block.reshape(1, groups_x, groups_y, piece, block.shape[2])
    return shaped.transpose(0, 2, 1, 3, 4).reshape(1, total_rows, block.shape[2])


def plain_body(old_master, old_first, old_second, new_grad, counts, old_owner, new_owner):
    experts = old_owner.shape[0]
    groups_x = lax.axis_size("gx")
    groups_y = lax.axis_size("gy")
    my_slot = lax.axis_index("gx") * groups_y + lax.axis_index("gy")
    slots = jnp.arange(experts, dtype=jnp.int32)
    onehot = new_owner[:, None] == slots[None, :]
    source = jnp.sum(jnp.where(onehot, old_owner[:, None], 0), axis=0)
    local_counts = counts[:, 0].astype(jnp.float32)
    by_rows = tuple(
        lax.all_to_all(state, "gx", split_axis=1, concat_axis=0, tiled=True)
        for state in (old_master, old_first, old_second)
    )
    permuted = tuple((jnp.take(state, source, axis=0) for state in by_rows))
    landed = lax.all_to_all(permuted, ("gx", "gy"), split_axis=0, concat_axis=1, tiled=True)
    arrived = tuple((reorder(state, groups_x, groups_y) for state in landed))
    totals = lax.psum(local_counts, ("gx", "gy"))
    slot_count = jnp.sum(jnp.where(new_owner == my_slot, totals, jnp.float32(0.0)))
    return adam_step(arrived[0], arrived[1], arrived[2], new_grad, slot_count)


def rehome_kernel(
    plan, old_owner_hbm, new_owner_hbm, owner_row_hbm, count_row, grad_hbm, old_m, old_f, old_s, moved, *scratch
):
    bands = len(plan.widths)
    chunks = bands * STATES
    by_rows = scratch[:chunks]
    staged, ready = scratch[chunks : chunks + bands], scratch[chunks + bands : chunks + 2 * bands]
    (
        source, old_owner, new_owner, owner_row, all_counts, grad,
        small_sem, grad_sem, local_sem, send1, recv1, send2, recv2, send_c, recv_c,
        row_in, up_in, mate_in, far_down, far_up,
    ) = scratch[chunks + 2 * bands :]
    olds = (old_m, old_f, old_s)
    groups_x, groups_y, experts, held, rows = plan.groups_x, plan.groups_y, plan.experts, plan.held, plan.rows
    devices = groups_x * groups_y
    splits = groups_x // plan.tiles
    planes = groups_y // PAIR
    half = planes // 2
    gx = lax.axis_index("gx")
    gy = lax.axis_index("gy")
    me = gx * groups_y + gy
    plane = gy // PAIR
    side = gy % PAIR
    mate = gy + 1 - 2 * side
    upper = plane // half
    has_low = plane > 0
    has_high = plane < planes - 1

    peers_x = [(gx + off) % groups_x for off in range(groups_x)]

    def signal(sem, px, py):
        pl.semaphore_signal(sem, inc=1, device_id=(px, py), device_id_type=MESH)

    barrier = pltpu.get_barrier_semaphore()
    for off in range(1, groups_x):
        signal(barrier, peers_x[off], gy)

    @pl.when(has_high)
    def _():
        signal(barrier, gx, gy + PAIR)
        pl.when(side == 0)(lambda: signal(barrier, gx, mate + PAIR))

    pl.when(side == 0)(lambda: signal(barrier, gx, mate))

    small = (
        pltpu.make_async_copy(old_owner_hbm, old_owner, small_sem),
        pltpu.make_async_copy(new_owner_hbm, new_owner, small_sem),
        pltpu.make_async_copy(owner_row_hbm, owner_row, small_sem),
        pltpu.make_async_copy(count_row, all_counts.at[me], small_sem),
    )
    grad_copy = pltpu.make_async_copy(grad_hbm, grad, grad_sem)

    def landed(ref, sem):
        pltpu.make_async_copy(ref, ref, sem).wait()

    def columns(band, part):
        start = (part % splits) * plan.span + plan.starts[band]
        return pl.ds(pl.multiple_of(start, LANES), plan.widths[band])

    def own_rows(band, state):
        return by_rows[band * STATES + state].at[pl.ds(gx * held, held)]

    def load(band, state, sem):
        for off in [*range(1, groups_x), 0]:
            part = peers_x[off]
            target = own_rows(band, state) if off == 0 else ready[band].at[state, off - 1]
            row = pl.ds(pl.multiple_of((part // splits) * SUBLANES, SUBLANES), SUBLANES)
            pltpu.make_async_copy(olds[state].at[:, row, columns(band, part)], target, sem).start()

    def first_sends(band, state):
        for off in range(1, groups_x):
            pltpu.make_async_remote_copy(
                src_ref=ready[band].at[state, off - 1],
                dst_ref=own_rows(band, state),
                send_sem=send1,
                recv_sem=recv1.at[band * STATES + state],
                device_id=(peers_x[off], gy),
                device_id_type=MESH,
            ).start()

    def loop(start, stop, fn):
        lax.fori_loop(start, stop, lambda k, carry: (fn(k), carry)[1], 0)

    load(0, 0, local_sem.at[0])
    for copy in small:
        copy.start()
    for band in range(bands):
        for state in range(STATES):
            if band or state:
                load(band, state, local_sem.at[1 + band])
    grad_copy.start()

    low = jnp.where(has_low, 1, 0)
    pl.semaphore_wait(barrier, groups_x - 1 + low + side * (1 + low))
    for off in range(1, groups_x):
        signal(row_in, peers_x[off], gy)

    landed(by_rows[0], local_sem.at[0])
    first_sends(0, 0)
    landed(staged[0].at[pl.ds(1, STATES - 1)], local_sem.at[1])
    for state in range(1, STATES):
        first_sends(0, state)
    for band in range(1, bands):
        landed(staged[band], local_sem.at[1 + band])
        for state in range(STATES):
            first_sends(band, state)

    for copy in small:
        copy.wait()
    owners = [new_owner[e] for e in range(experts)]
    places = [old_owner[e] for e in range(experts)]

    def find(slot, carry):
        total = jnp.int32(0)
        for e in range(experts):
            total = total + jnp.where(owners[e] == slot, places[e], 0)
        source[slot] = total
        return carry

    pl.semaphore_wait(row_in, groups_x - 1)
    pl.when(side == 1)(lambda: signal(mate_in, gx, mate))

    lax.fori_loop(0, experts // 2, find, 0)

    pl.when(side == 0)(lambda: pl.semaphore_wait(mate_in, 1))
    pl.when(has_low)(lambda: signal(up_in, gx, gy - PAIR))

    lax.fori_loop(experts // 2, experts, find, 0)

    def meet_upper():
        pl.semaphore_wait(up_in, 1)
        if planes > 2:
            pl.when(has_low)(lambda: signal(far_up.at[0], gx, gy - PAIR))
            pl.when(has_low)(lambda: signal(far_down.at[0], gx, gy + PAIR))

    pl.when(upper == 0)(meet_upper)

    def landing(band, state):
        row = pl.multiple_of(gy * rows + (gx // splits) * SUBLANES, SUBLANES)
        return moved.at[state, pl.ds(row, SUBLANES), columns(band, gx)]

    def send(chunk, px, py):
        band, state = divmod(chunk, STATES)
        pltpu.make_async_remote_copy(
            src_ref=staged[band].at[state, px * groups_y + py],
            dst_ref=landing(band, state),
            send_sem=send2,
            recv_sem=recv2.at[band],
            device_id=(px, py),
            device_id_type=MESH,
        ).start()

    def send_count(px, py):
        pltpu.make_async_remote_copy(
            src_ref=all_counts.at[me],
            dst_ref=all_counts.at[me],
            send_sem=send_c,
            recv_sem=recv_c,
            device_id=(px, py),
            device_id_type=MESH,
        ).start()

    def to_plane(fn, target):
        for pair in range(PAIR):
            py = target * PAIR + (side + pair + 1) % PAIR
            for px in peers_x[1:] + peers_x[:1]:
                fn(px, py)

    def to_own_plane(fn):
        for px in peers_x:
            fn(px, mate)
        for px in peers_x[1:]:
            fn(px, gy)

    def to_distance(fns, far):
        @pl.when(plane >= far)
        def _():
            if far >= 2:
                pl.semaphore_wait(far_down.at[far - 2], 1)
                if far < planes - 1:
                    pl.when(has_high)(lambda: signal(far_down.at[far - 1], gx, gy + PAIR))
            for fn in fns:
                to_plane(fn, plane - far)

        @pl.when(plane < planes - far)
        def _():
            if far >= 2:
                pl.semaphore_wait(far_up.at[far - 2], 1)
                if far < planes - 1:
                    pl.when(has_low)(lambda: signal(far_up.at[far - 1], gx, gy - PAIR))
            for fn in fns:
                to_plane(fn, plane + far)

    def to_known(fn, far):
        for k in range(1, far + 1):
            pl.when(plane >= k)(functools.partial(to_plane, fn, plane - k))
            pl.when(plane < planes - k)(functools.partial(to_plane, fn, plane + k))

    def spread(fn):
        for k in range(half):
            to_plane(fn, upper * k + (1 - upper) * (planes - 1 - k))
        for k in range(1, half):
            to_plane(fn, upper * half + (plane + k) % half)
        to_own_plane(fn)

    def stage(chunk):
        band, state = divmod(chunk, STATES)
        landed(ready[band].at[state], recv1.at[chunk])

        def one(slot, carry):
            staged[band][state, slot] = by_rows[chunk][source[slot]]
            return carry

        lax.fori_loop(0, experts, one, 0, unroll=4)
        landing(band, state)[...] = by_rows[chunk][source[me]]

    early = planes - 1
    for chunk in range(early):
        stage(chunk)
        fn = functools.partial(send, chunk)
        if chunk == 0:
            pl.when(has_low)(lambda: to_plane(fn, plane - 1))
            pl.when(jnp.logical_and(upper == 1, has_high))(meet_upper)
            pl.when(has_high)(lambda: to_plane(fn, plane + 1))
        else:
            to_known(fn, chunk)
            to_distance([functools.partial(send, k) for k in range(chunk + 1)], chunk + 1)
        to_own_plane(fn)

    def step(chunk):
        stage(chunk)
        spread(functools.partial(send, chunk))

    hold = jnp.where(upper == 1, HOLD_LOW, HOLD_HIGH)
    first_plane = (1 - upper) * half

    def eager(chunk):
        stage(chunk)
        fn = functools.partial(send, chunk)
        to_plane(fn, first_plane)
        for k in range(1, half):
            pl.when(chunk < chunks - hold)(functools.partial(to_plane, fn, first_plane + k))
        to_own_plane(fn)
        for k in range(1, half):
            to_plane(fn, upper * half + (plane + k) % half)

    def held_back(chunk):
        for k in range(1, half):
            to_plane(functools.partial(send, chunk), first_plane + k)

    for chunk in range(early, chunks):
        (step if chunk < chunks - max(HOLD_LOW, HOLD_HIGH) else eager)(chunk)
        if chunk == early:
            spread(send_count)
    for chunk in range(chunks - max(HOLD_LOW, HOLD_HIGH), chunks):
        pl.when(chunk >= chunks - hold)(functools.partial(held_back, chunk))

    others = all_counts.at[pl.ds(0, devices - 1)]
    landed(others, recv_c)
    grad_copy.wait()
    totals = jnp.sum(all_counts[...].astype(jnp.float32), axis=0)
    slot_count = jnp.sum(jnp.where(owner_row[...] == me, totals, 0.0), axis=1, keepdims=True)

    per_token = 1.0 / slot_count

    for band, width in enumerate(plan.widths):
        landed(staged[band].at[:, pl.ds(0, devices - 1)], recv2.at[band])

        def adam(step, carry):
            row = pl.ds(pl.multiple_of(step * ADAM_ROWS, ADAM_ROWS), ADAM_ROWS)
            for part in range(splits):
                col = pl.ds(part * plan.span + plan.starts[band], width)
                fresh = adam_scaled(
                    moved[0, row, col], moved[1, row, col], moved[2, row, col], grad[0, row, col], per_token
                )
                for k in range(STATES):
                    moved[k, row, col] = fresh[k]
            return carry

        lax.fori_loop(0, rows * groups_y // ADAM_ROWS, adam, 0, unroll=2)

    landed(others, send_c)
    for band in range(bands):
        landed(ready[band], send1)
        landed(staged[band].at[:, pl.ds(0, devices - 1)], send2)


def publish_kernel(moved, master, first, second, sem):
    rows = master.shape[1] // PUBLISHED
    copies = [
        pltpu.make_async_copy(moved.at[pl.ds(k, 1), pl.ds(part * rows, rows)], out.at[:, pl.ds(part * rows, rows)], sem)
        for k, out in enumerate((master, first, second))
        for part in range(PUBLISHED)
    ]
    for copy in copies:
        copy.start()
    for copy in copies:
        copy.wait()


class Plan:
    def __init__(self, groups_x, groups_y, shape, experts):
        self.groups_x, self.groups_y, self.experts = groups_x, groups_y, experts
        self.held, self.rows, cols = shape
        self.fits = False
        if self.rows % SUBLANES or experts != groups_x * groups_y or groups_y % (2 * PAIR) or groups_y == 2 * PAIR:
            return
        self.tiles = self.rows // SUBLANES
        if groups_x % self.tiles or self.rows * groups_y % ADAM_ROWS:
            return
        self.span = cols // (groups_x // self.tiles)
        if self.span % LANES or cols % (groups_x // self.tiles):
            return
        blocks = self.span // LANES
        widths = [1, *[BAND] * ((blocks - 1) // BAND), (blocks - 1) % BAND]
        widths = WIDTHS if sum(WIDTHS) == blocks else widths
        self.widths = [LANES * width for width in widths if width]
        self.starts = [sum(self.widths[:k]) for k in range(len(self.widths))]
        self.fits = len(self.widths) * STATES > groups_y // PAIR + max(HOLD_LOW, HOLD_HIGH)


def kernel_body(plan, old_master, old_first, old_second, new_grad, counts, old_owner, new_owner):
    experts = plan.experts
    devices = plan.groups_x * plan.groups_y
    bands = len(plan.widths)
    rows, cols = plan.rows * plan.groups_y, old_master.shape[2]
    vmem = pl.BlockSpec(memory_space=pltpu.VMEM)
    hbm = pl.BlockSpec(memory_space=pltpu.HBM)
    far = max(plan.groups_y // PAIR - 2, 1)
    by_rows = [pltpu.VMEM((experts, SUBLANES, width), jnp.float32) for width in plan.widths for _ in range(STATES)]
    staged = [pltpu.VMEM((STATES, experts, SUBLANES, width), jnp.float32) for width in plan.widths]
    ready = [
        pltpu.VMEM((STATES, plan.groups_x - 1, plan.held, SUBLANES, width), jnp.float32) for width in plan.widths
    ]
    row = new_owner.reshape(1, experts)
    operands = (
        old_owner, new_owner, row, counts.reshape(1, experts), new_grad, old_master, old_first, old_second,
    )
    kept = [pltpu.with_memory_space_constraint(array, pltpu.HBM) for array in operands]
    moved = pl.pallas_call(
        functools.partial(rehome_kernel, plan),
        out_shape=jax.ShapeDtypeStruct((STATES, rows, cols), jnp.float32),
        in_specs=[hbm] * 8,
        out_specs=vmem,
        scratch_shapes=by_rows
        + staged
        + ready
        + [
            pltpu.SMEM((experts,), jnp.int32),
            pltpu.SMEM((experts,), jnp.int32),
            pltpu.SMEM((experts,), jnp.int32),
            pltpu.VMEM((1, experts), jnp.int32),
            pltpu.VMEM((devices, 1, experts), jnp.int32),
            pltpu.VMEM((1, rows, cols), new_grad.dtype),
            pltpu.SemaphoreType.DMA,
            pltpu.SemaphoreType.DMA,
            pltpu.SemaphoreType.DMA((bands + 1,)),
            pltpu.SemaphoreType.DMA,
            pltpu.SemaphoreType.DMA((bands * STATES,)),
            pltpu.SemaphoreType.DMA,
            pltpu.SemaphoreType.DMA((bands,)),
            pltpu.SemaphoreType.DMA,
            pltpu.SemaphoreType.DMA,
            pltpu.SemaphoreType.REGULAR,
            pltpu.SemaphoreType.REGULAR,
            pltpu.SemaphoreType.REGULAR,
            pltpu.SemaphoreType.REGULAR((far,)),
            pltpu.SemaphoreType.REGULAR((far,)),
        ],
        compiler_params=pltpu.CompilerParams(collective_id=0, has_side_effects=True, vmem_limit_bytes=VMEM_GRANT),
    )(*kept)
    return pl.pallas_call(
        publish_kernel,
        out_shape=[jax.ShapeDtypeStruct((1, rows, cols), jnp.float32)] * STATES,
        in_specs=[pl.BlockSpec(memory_space=pl.ANY)],
        out_specs=[hbm] * STATES,
        scratch_shapes=[pltpu.SemaphoreType.DMA],
        compiler_params=pltpu.CompilerParams(vmem_limit_bytes=1 << 20),
    )(moved)


def body(old_master, old_first, old_second, new_grad, counts, old_owner, new_owner):
    plan = Plan(lax.axis_size("gx"), lax.axis_size("gy"), old_master.shape, old_owner.shape[0])
    if not plan.fits:
        return plain_body(old_master, old_first, old_second, new_grad, counts, old_owner, new_owner)
    return kernel_body(plan, old_master, old_first, old_second, new_grad, counts, old_owner, new_owner)


def solution(mesh):
    placed = (
        P("gx", "gy", None),
        P("gx", "gy", None),
        P("gx", "gy", None),
        P(("gx", "gy"), None, None),
        P(None, ("gx", "gy")),
        P(),
        P(),
    )
    return jax.shard_map(
        body,
        mesh=mesh,
        in_specs=placed,
        out_specs=(P(("gx", "gy"), None, None),) * 3,
        check_vma=False,
    )
```

```python
import functools

import jax
import jax.numpy as jnp
from jax import lax
from jax.experimental import pallas as pl
from jax.experimental.pallas import tpu as pltpu
from jax.sharding import PartitionSpec as P

first_correction = 1.0 - 0.9**10
second_correction = 1.0 - 0.999**10
MESH = pl.DeviceIdType.MESH
LANES = 128
VMEM_GRANT = 24 << 20
SUBLANES = 8
PAIR = 2
STATES = 3
MASTER, FIRST, SECOND = range(STATES)
TURNS = (FIRST, SECOND, MASTER)
ADAM_ROWS = 16
PUBLISHED = 4
BAND = 2
WIDTHS = (1, 2, 3)


def adam_step(master, first, second, grad, slot_count):
    scaled = grad.astype(jnp.float32) / slot_count
    new_first = 0.9 * first + 0.1 * scaled
    new_second = 0.999 * second + 0.001 * scaled * scaled
    step_dir = new_first / first_correction / (jnp.sqrt(new_second / second_correction) + 1e-08)
    new_master = master - 0.01 * (step_dir + 0.1 * master)
    return (new_master, new_first, new_second)


def adam_direction(first, second, grad, per_token):
    scaled = grad.astype(jnp.float32) * per_token
    new_first = 0.9 * first + 0.1 * scaled
    new_second = 0.999 * second + 0.001 * scaled * scaled
    step_dir = new_first * (1.0 / first_correction) / (jnp.sqrt(new_second * (1.0 / second_correction)) + 1e-08)
    return (new_first, new_second, step_dir)


def adam_weights(master, step_dir):
    return master - 0.01 * (step_dir + 0.1 * master)


def reorder(block, groups_x, groups_y):
    total_rows = block.shape[1]
    piece = total_rows // (groups_x * groups_y)
    shaped = block.reshape(1, groups_x, groups_y, piece, block.shape[2])
    return shaped.transpose(0, 2, 1, 3, 4).reshape(1, total_rows, block.shape[2])


def plain_body(old_master, old_first, old_second, new_grad, counts, old_owner, new_owner):
    experts = old_owner.shape[0]
    groups_x = lax.axis_size("gx")
    groups_y = lax.axis_size("gy")
    my_slot = lax.axis_index("gx") * groups_y + lax.axis_index("gy")
    slots = jnp.arange(experts, dtype=jnp.int32)
    onehot = new_owner[:, None] == slots[None, :]
    source = jnp.sum(jnp.where(onehot, old_owner[:, None], 0), axis=0)
    local_counts = counts[:, 0].astype(jnp.float32)
    by_rows = tuple(
        lax.all_to_all(state, "gx", split_axis=1, concat_axis=0, tiled=True)
        for state in (old_master, old_first, old_second)
    )
    permuted = tuple((jnp.take(state, source, axis=0) for state in by_rows))
    landed = lax.all_to_all(permuted, ("gx", "gy"), split_axis=0, concat_axis=1, tiled=True)
    arrived = tuple((reorder(state, groups_x, groups_y) for state in landed))
    totals = lax.psum(local_counts, ("gx", "gy"))
    slot_count = jnp.sum(jnp.where(new_owner == my_slot, totals, jnp.float32(0.0)))
    return adam_step(arrived[0], arrived[1], arrived[2], new_grad, slot_count)


def rehome_kernel(
    plan, old_owner_hbm, new_owner_hbm, owner_row_hbm, count_row, grad_hbm, old_m, old_f, old_s, moved, *scratch
):
    bands = len(plan.widths)
    chunks = bands * STATES
    by_rows = scratch[:chunks]
    staged, ready = scratch[chunks : chunks + bands], scratch[chunks + bands : chunks + 2 * bands]
    (
        source, old_owner, new_owner, owner_row, row_counts, all_counts, grad, steps,
        small_sem, grad_sem, local_sem, send1, recv1, send2, recv2, send_c, recv_c,
        row_in, up_in, mate_in, far_down, far_up,
    ) = scratch[chunks + 2 * bands :]
    olds = (old_m, old_f, old_s)
    groups_x, groups_y, experts, held, rows = plan.groups_x, plan.groups_y, plan.experts, plan.held, plan.rows
    devices = groups_x * groups_y
    splits = groups_x // plan.tiles
    planes = groups_y // PAIR
    half = planes // 2
    gx = lax.axis_index("gx")
    gy = lax.axis_index("gy")
    me = gx * groups_y + gy
    plane = gy // PAIR
    side = gy % PAIR
    mate = gy + 1 - 2 * side
    upper = plane // half
    has_low = plane > 0
    has_high = plane < planes - 1

    peers_x = [(gx + off) % groups_x for off in range(groups_x)]

    def signal(sem, px, py):
        pl.semaphore_signal(sem, inc=1, device_id=(px, py), device_id_type=MESH)

    barrier = pltpu.get_barrier_semaphore()
    for off in range(1, groups_x):
        signal(barrier, peers_x[off], gy)

    @pl.when(has_high)
    def _():
        signal(barrier, gx, gy + PAIR)
        pl.when(side == 0)(lambda: signal(barrier, gx, mate + PAIR))

    pl.when(side == 0)(lambda: signal(barrier, gx, mate))

    small = (
        pltpu.make_async_copy(old_owner_hbm, old_owner, small_sem),
        pltpu.make_async_copy(new_owner_hbm, new_owner, small_sem),
        pltpu.make_async_copy(owner_row_hbm, owner_row, small_sem),
        pltpu.make_async_copy(count_row, row_counts.at[gx], small_sem),
    )
    grad_copy = pltpu.make_async_copy(grad_hbm, grad, grad_sem)

    def landed(ref, sem):
        pltpu.make_async_copy(ref, ref, sem).wait()

    def columns(band, part):
        start = (part % splits) * plan.span + plan.starts[band]
        return pl.ds(pl.multiple_of(start, LANES), plan.widths[band])

    def own_rows(band, state):
        return by_rows[band * STATES + state].at[pl.ds(gx * held, held)]

    def load(band, state, sem):
        for off in [*range(1, groups_x), 0]:
            part = peers_x[off]
            target = own_rows(band, state) if off == 0 else ready[band].at[state, off - 1]
            row = pl.ds(pl.multiple_of((part // splits) * SUBLANES, SUBLANES), SUBLANES)
            pltpu.make_async_copy(olds[TURNS[state]].at[:, row, columns(band, part)], target, sem).start()

    def first_sends(band, state):
        for off in range(1, groups_x):
            pltpu.make_async_remote_copy(
                src_ref=ready[band].at[state, off - 1],
                dst_ref=own_rows(band, state),
                send_sem=send1,
                recv_sem=recv1.at[band * STATES + state],
                device_id=(peers_x[off], gy),
                device_id_type=MESH,
            ).start()

    def loop(start, stop, fn):
        lax.fori_loop(start, stop, lambda k, carry: (fn(k), carry)[1], 0)

    def count_copy(rows, k, sem, px, py):
        return pltpu.make_async_remote_copy(
            src_ref=rows.at[k],
            dst_ref=rows.at[k],
            send_sem=send_c.at[sem],
            recv_sem=recv_c.at[sem],
            device_id=(px, py),
            device_id_type=MESH,
        )

    load(0, 0, local_sem.at[0])
    for copy in small:
        copy.start()
    for band in range(bands):
        for state in range(STATES):
            if band or state:
                load(band, state, local_sem.at[1 + band])
    grad_copy.start()

    low = jnp.where(has_low, 1, 0)
    pl.semaphore_wait(barrier, groups_x - 1 + low + side * (1 + low))
    for off in range(1, groups_x):
        signal(row_in, peers_x[off], gy)

    landed(by_rows[0], local_sem.at[0])
    first_sends(0, 0)
    for copy in small:
        copy.wait()
    for off in range(1, groups_x):
        count_copy(row_counts, gx, 0, peers_x[off], gy).start()
    landed(staged[0].at[pl.ds(1, STATES - 1)], local_sem.at[1])
    for state in range(1, STATES):
        first_sends(0, state)
    for band in range(1, bands):
        landed(staged[band], local_sem.at[1 + band])
        for state in range(STATES):
            first_sends(band, state)

    owners = [new_owner[e] for e in range(experts)]
    places = [old_owner[e] for e in range(experts)]

    def find(slot, carry):
        total = jnp.int32(0)
        for e in range(experts):
            total = total + jnp.where(owners[e] == slot, places[e], 0)
        source[slot] = total
        return carry

    pl.semaphore_wait(row_in, groups_x - 1)
    pl.when(side == 1)(lambda: signal(mate_in, gx, mate))

    lax.fori_loop(0, experts // 2, find, 0)

    pl.when(side == 0)(lambda: pl.semaphore_wait(mate_in, 1))
    pl.when(has_low)(lambda: signal(up_in, gx, gy - PAIR))

    lax.fori_loop(experts // 2, experts, find, 0)

    def meet_upper():
        pl.semaphore_wait(up_in, 1)
        if planes > 2:
            pl.when(has_low)(lambda: signal(far_up.at[0], gx, gy - PAIR))
            pl.when(has_low)(lambda: signal(far_down.at[0], gx, gy + PAIR))

    pl.when(upper == 0)(meet_upper)

    def landing(band, state):
        row = pl.multiple_of(gy * rows + (gx // splits) * SUBLANES, SUBLANES)
        return moved.at[TURNS[state], pl.ds(row, SUBLANES), columns(band, gx)]

    def send(chunk, px, py):
        band, state = divmod(chunk, STATES)
        pltpu.make_async_remote_copy(
            src_ref=staged[band].at[state, px * groups_y + py],
            dst_ref=landing(band, state),
            send_sem=send2,
            recv_sem=recv2.at[2 * band + state // (STATES - 1)],
            device_id=(px, py),
            device_id_type=MESH,
        ).start()

    def send_counts():
        landed(row_counts.at[pl.ds(0, groups_x - 1)], recv_c.at[0])
        all_counts[gy] = jnp.sum(row_counts[...], axis=0)
        for off in range(1, groups_y):
            count_copy(all_counts, gy, 1, gx, (gy + off) % groups_y).start()

    def to_plane(fn, target):
        for pair in range(PAIR):
            py = target * PAIR + (side + pair + 1) % PAIR
            for px in peers_x[1:] + peers_x[:1]:
                fn(px, py)

    def to_own_plane(fn):
        for px in peers_x:
            fn(px, mate)
        for px in peers_x[1:]:
            fn(px, gy)

    def to_lower(fns, far):
        pl.semaphore_wait(far_down.at[far - 2], 1)
        if far < planes - 1:
            pl.when(has_high)(lambda: signal(far_down.at[far - 1], gx, gy + PAIR))
        for fn in fns:
            to_plane(fn, plane - far)

    def reach_down(fn):
        pl.semaphore_wait(far_down.at[0], 1)
        to_plane(fn, plane - 2)

    def to_upper(fns, far):
        pl.semaphore_wait(far_up.at[far - 2], 1)
        if far < planes - 1:
            pl.when(has_low)(lambda: signal(far_up.at[far - 1], gx, gy - PAIR))
        for fn in fns:
            to_plane(fn, plane + far)

    def spread(fn):
        for k in range(half):
            to_plane(fn, upper * k + (1 - upper) * (planes - 1 - k))
        for k in range(1, half):
            to_plane(fn, upper * half + (plane + k) % half)
        to_own_plane(fn)

    def stage(chunk):
        band, state = divmod(chunk, STATES)
        landed(ready[band].at[state], recv1.at[chunk])

        def one(slot, carry):
            staged[band][state, slot] = by_rows[chunk][source[slot]]
            return carry

        lax.fori_loop(0, experts, one, 0, unroll=4)
        landing(band, state)[...] = by_rows[chunk][source[me]]

    early = planes - 1
    for chunk in range(early):
        stage(chunk)
        fn = functools.partial(send, chunk)
        if chunk == 0:
            pl.when(has_low)(lambda: to_plane(fn, plane - 1))
            pl.when(upper == 1)(functools.partial(reach_down, fn))
            pl.when(jnp.logical_and(upper == 1, has_high))(meet_upper)
            if planes > 3:
                pl.when(jnp.logical_and(upper == 1, has_high))(lambda: signal(far_down.at[1], gx, gy + PAIR))
            pl.when(has_high)(lambda: to_plane(fn, plane + 1))
        else:
            fns = [functools.partial(send, k) for k in range(chunk + 1)]
            far = chunk + 1
            for k in range(1, far):
                pl.when(plane >= k)(functools.partial(to_plane, fn, plane - k))
                pl.when(plane < planes - k)(functools.partial(to_plane, fn, plane + k))
            if far == 2:
                pl.when(upper == 1)(lambda: to_plane(fn, plane - 2))
                pl.when(jnp.logical_and(upper == 0, plane >= far))(lambda: to_lower(fns, far))
            else:
                pl.when(plane >= far)(lambda: to_lower(fns, far))
            pl.when(plane < planes - far)(lambda: to_upper(fns, far))
        to_own_plane(fn)

    def step(chunk):
        stage(chunk)
        spread(functools.partial(send, chunk))

    for chunk in range(early, chunks):
        step(chunk)
        if chunk == early:
            send_counts()

    landed(all_counts.at[pl.ds(0, groups_y - 1)], recv_c.at[1])
    grad_copy.wait()
    totals = jnp.sum(all_counts[...].astype(jnp.float32), axis=0)
    slot_count = jnp.sum(jnp.where(owner_row[...] == me, totals, 0.0), axis=1, keepdims=True)
    per_token = 1.0 / slot_count

    def tiles(band, fn):
        def one(step, carry):
            row = pl.ds(pl.multiple_of(step * ADAM_ROWS, ADAM_ROWS), ADAM_ROWS)
            for part in range(splits):
                width = plan.widths[band]
                fn(row, pl.ds(part * plan.span + plan.starts[band], width))
            return carry

        lax.fori_loop(0, rows * groups_y // ADAM_ROWS, one, 0, unroll=2)

    def moments(row, col):
        moved[FIRST, row, col], moved[SECOND, row, col], steps[row, col] = adam_direction(
            moved[FIRST, row, col], moved[SECOND, row, col], grad[0, row, col], per_token
        )

    def weights(row, col):
        moved[MASTER, row, col] = adam_weights(moved[MASTER, row, col], steps[row, col])

    for band in range(bands):
        landed(staged[band].at[pl.ds(0, STATES - 1), pl.ds(0, devices - 1)], recv2.at[2 * band])
        tiles(band, moments)
        landed(staged[band].at[0, pl.ds(0, devices - 1)], recv2.at[2 * band + 1])
        tiles(band, weights)

    landed(row_counts.at[pl.ds(0, groups_x - 1)], send_c.at[0])
    landed(all_counts.at[pl.ds(0, groups_y - 1)], send_c.at[1])
    for band in range(bands):
        landed(ready[band], send1)
        landed(staged[band].at[:, pl.ds(0, devices - 1)], send2)


def publish_kernel(moved, master, first, second, sem):
    rows = master.shape[1] // PUBLISHED
    copies = [
        pltpu.make_async_copy(moved.at[pl.ds(k, 1), pl.ds(part * rows, rows)], out.at[:, pl.ds(part * rows, rows)], sem)
        for k, out in enumerate((master, first, second))
        for part in range(PUBLISHED)
    ]
    for copy in copies:
        copy.start()
    for copy in copies:
        copy.wait()


class Plan:
    def __init__(self, groups_x, groups_y, shape, experts):
        self.groups_x, self.groups_y, self.experts = groups_x, groups_y, experts
        self.held, self.rows, cols = shape
        self.fits = False
        if self.rows % SUBLANES or experts != groups_x * groups_y or groups_y % (2 * PAIR) or groups_y == 2 * PAIR:
            return
        self.tiles = self.rows // SUBLANES
        if groups_x % self.tiles or self.rows * groups_y % ADAM_ROWS:
            return
        self.span = cols // (groups_x // self.tiles)
        if self.span % LANES or cols % (groups_x // self.tiles):
            return
        blocks = self.span // LANES
        widths = [1, *[BAND] * ((blocks - 1) // BAND), (blocks - 1) % BAND]
        widths = WIDTHS if sum(WIDTHS) == blocks else widths
        self.widths = [LANES * width for width in widths if width]
        self.starts = [sum(self.widths[:k]) for k in range(len(self.widths))]
        self.fits = len(self.widths) * STATES > groups_y // PAIR


def kernel_body(plan, old_master, old_first, old_second, new_grad, counts, old_owner, new_owner):
    experts = plan.experts
    devices = plan.groups_x * plan.groups_y
    bands = len(plan.widths)
    rows, cols = plan.rows * plan.groups_y, old_master.shape[2]
    vmem = pl.BlockSpec(memory_space=pltpu.VMEM)
    hbm = pl.BlockSpec(memory_space=pltpu.HBM)
    far = max(plan.groups_y // PAIR - 2, 1)
    by_rows = [pltpu.VMEM((experts, SUBLANES, width), jnp.float32) for width in plan.widths for _ in range(STATES)]
    staged = [pltpu.VMEM((STATES, experts, SUBLANES, width), jnp.float32) for width in plan.widths]
    ready = [
        pltpu.VMEM((STATES, plan.groups_x - 1, plan.held, SUBLANES, width), jnp.float32) for width in plan.widths
    ]
    row = new_owner.reshape(1, experts)
    operands = (
        old_owner, new_owner, row, counts.reshape(1, experts), new_grad, old_master, old_first, old_second,
    )
    kept = [pltpu.with_memory_space_constraint(array, pltpu.HBM) for array in operands]
    moved = pl.pallas_call(
        functools.partial(rehome_kernel, plan),
        out_shape=jax.ShapeDtypeStruct((STATES, rows, cols), jnp.float32),
        in_specs=[hbm] * 8,
        out_specs=vmem,
        scratch_shapes=by_rows
        + staged
        + ready
        + [
            pltpu.SMEM((experts,), jnp.int32),
            pltpu.SMEM((experts,), jnp.int32),
            pltpu.SMEM((experts,), jnp.int32),
            pltpu.VMEM((1, experts), jnp.int32),
            pltpu.VMEM((plan.groups_x, 1, experts), jnp.int32),
            pltpu.VMEM((plan.groups_y, 1, experts), jnp.int32),
            pltpu.VMEM((1, rows, cols), new_grad.dtype),
            pltpu.VMEM((rows, cols), jnp.float32),
            pltpu.SemaphoreType.DMA,
            pltpu.SemaphoreType.DMA,
            pltpu.SemaphoreType.DMA((bands + 1,)),
            pltpu.SemaphoreType.DMA,
            pltpu.SemaphoreType.DMA((bands * STATES,)),
            pltpu.SemaphoreType.DMA,
            pltpu.SemaphoreType.DMA((2 * bands,)),
            pltpu.SemaphoreType.DMA((2,)),
            pltpu.SemaphoreType.DMA((2,)),
            pltpu.SemaphoreType.REGULAR,
            pltpu.SemaphoreType.REGULAR,
            pltpu.SemaphoreType.REGULAR,
            pltpu.SemaphoreType.REGULAR((far,)),
            pltpu.SemaphoreType.REGULAR((far,)),
        ],
        compiler_params=pltpu.CompilerParams(collective_id=0, has_side_effects=True, vmem_limit_bytes=VMEM_GRANT),
    )(*kept)
    return pl.pallas_call(
        publish_kernel,
        out_shape=[jax.ShapeDtypeStruct((1, rows, cols), jnp.float32)] * STATES,
        in_specs=[pl.BlockSpec(memory_space=pl.ANY)],
        out_specs=[hbm] * STATES,
        scratch_shapes=[pltpu.SemaphoreType.DMA],
        compiler_params=pltpu.CompilerParams(vmem_limit_bytes=1 << 20),
    )(moved)


def body(old_master, old_first, old_second, new_grad, counts, old_owner, new_owner):
    plan = Plan(lax.axis_size("gx"), lax.axis_size("gy"), old_master.shape, old_owner.shape[0])
    if not plan.fits:
        return plain_body(old_master, old_first, old_second, new_grad, counts, old_owner, new_owner)
    return kernel_body(plan, old_master, old_first, old_second, new_grad, counts, old_owner, new_owner)


def solution(mesh):
    placed = (
        P("gx", "gy", None),
        P("gx", "gy", None),
        P("gx", "gy", None),
        P(("gx", "gy"), None, None),
        P(None, ("gx", "gy")),
        P(),
        P(),
    )
    return jax.shard_map(
        body,
        mesh=mesh,
        in_specs=placed,
        out_specs=(P(("gx", "gy"), None, None),) * 3,
        check_vma=False,
    )
```

```python
import functools
from typing import NamedTuple

import jax
import jax.numpy as jnp
from jax import lax
from jax.experimental import pallas as pl
from jax.experimental.pallas import tpu as pltpu
from jax.sharding import PartitionSpec as P

first_correction = 1.0 - 0.9**10
second_correction = 1.0 - 0.999**10
MESH = pl.DeviceIdType.MESH
LANES = 128
VMEM_GRANT = 24 << 20
SUBLANES = 8
PAIR = 2
STATES = 3
MASTER, FIRST, SECOND = range(STATES)
TURNS = (FIRST, SECOND, MASTER)
FIRST_LOADS = 2
EARLY_BANDS, LAST_MOMENTS, LAST_WEIGHTS = range(3)
ADAM_ROWS = 16
PUBLISHED = 4
BAND = 2
WIDTHS = (1, 2, 3)


def adam_step(master, first, second, grad, slot_count):
    scaled = grad.astype(jnp.float32) / slot_count
    new_first = 0.9 * first + 0.1 * scaled
    new_second = 0.999 * second + 0.001 * scaled * scaled
    step_dir = new_first / first_correction / (jnp.sqrt(new_second / second_correction) + 1e-08)
    new_master = master - 0.01 * (step_dir + 0.1 * master)
    return (new_master, new_first, new_second)


def adam_direction(first, second, grad, per_token):
    scaled = grad.astype(jnp.float32) * per_token
    new_first = 0.9 * first + 0.1 * scaled
    new_second = 0.999 * second + 0.001 * scaled * scaled
    step_dir = new_first * (1.0 / first_correction) / (jnp.sqrt(new_second * (1.0 / second_correction)) + 1e-08)
    return (new_first, new_second, step_dir)


def adam_weights(master, step_dir):
    return master - 0.01 * (step_dir + 0.1 * master)


def reorder(block, groups_x, groups_y):
    total_rows = block.shape[1]
    piece = total_rows // (groups_x * groups_y)
    shaped = block.reshape(1, groups_x, groups_y, piece, block.shape[2])
    return shaped.transpose(0, 2, 1, 3, 4).reshape(1, total_rows, block.shape[2])


def plain_body(old_master, old_first, old_second, new_grad, counts, old_owner, new_owner):
    experts = old_owner.shape[0]
    groups_x = lax.axis_size("gx")
    groups_y = lax.axis_size("gy")
    my_slot = lax.axis_index("gx") * groups_y + lax.axis_index("gy")
    slots = jnp.arange(experts, dtype=jnp.int32)
    onehot = new_owner[:, None] == slots[None, :]
    source = jnp.sum(jnp.where(onehot, old_owner[:, None], 0), axis=0)
    local_counts = counts[:, 0].astype(jnp.float32)
    by_rows = tuple(
        lax.all_to_all(state, "gx", split_axis=1, concat_axis=0, tiled=True)
        for state in (old_master, old_first, old_second)
    )
    permuted = tuple((jnp.take(state, source, axis=0) for state in by_rows))
    landed = lax.all_to_all(permuted, ("gx", "gy"), split_axis=0, concat_axis=1, tiled=True)
    arrived = tuple((reorder(state, groups_x, groups_y) for state in landed))
    totals = lax.psum(local_counts, ("gx", "gy"))
    slot_count = jnp.sum(jnp.where(new_owner == my_slot, totals, jnp.float32(0.0)))
    return adam_step(arrived[0], arrived[1], arrived[2], new_grad, slot_count)


def rehome_kernel(
    plan, old_owner_hbm, new_owner_hbm, owner_row_hbm, count_row, grad_hbm, old_m, old_f, old_s, moved, *scratch
):
    chunks = len(plan.chunks)
    by_rows, staged, ready = (scratch[k * chunks : (k + 1) * chunks] for k in range(3))
    (
        source, old_owner, new_owner, owner_row, row_counts, all_counts, grad, steps, sizes,
        small_sem, grad_sem, local_sem, sent, recv1, recv2, recv_c,
        row_in, up_in, mate_in, far_up,
    ) = scratch[3 * chunks :]
    olds = (old_m, old_f, old_s)
    groups_x, groups_y, experts, held, rows = plan.groups_x, plan.groups_y, plan.experts, plan.held, plan.rows
    devices = groups_x * groups_y
    splits = groups_x // plan.tiles
    planes = groups_y // PAIR
    half = planes // 2
    gx = lax.axis_index("gx")
    gy = lax.axis_index("gy")
    me = gx * groups_y + gy
    plane = gy // PAIR
    side = gy % PAIR
    mate = gy + 1 - 2 * side
    upper = plane // half
    has_low = plane > 0
    has_high = plane < planes - 1

    peers_x = [(gx + off) % groups_x for off in range(groups_x)]

    def signal(sem, px, py):
        pl.semaphore_signal(sem, inc=1, device_id=(px, py), device_id_type=MESH)

    barrier = pltpu.get_barrier_semaphore()
    for off in range(1, groups_x):
        signal(barrier, peers_x[off], gy)

    def greet(k):
        signal(barrier, gx, gy + k * PAIR)
        pl.when(side == 0)(lambda: signal(barrier, gx, mate + k * PAIR))

    for k in range(1, planes):
        pl.when(plane + k < planes)(functools.partial(greet, k))

    pl.when(side == 0)(lambda: signal(barrier, gx, mate))

    small = (
        pltpu.make_async_copy(old_owner_hbm, old_owner, small_sem),
        pltpu.make_async_copy(new_owner_hbm, new_owner, small_sem),
        pltpu.make_async_copy(owner_row_hbm, owner_row, small_sem),
        pltpu.make_async_copy(count_row, row_counts.at[gx], small_sem),
    )
    grad_copy = pltpu.make_async_copy(grad_hbm, grad, grad_sem)

    def landed(ref, sem):
        pltpu.make_async_copy(ref, ref, sem).wait()

    def columns(chunk, part):
        start = (part % splits) * plan.span + plan.chunks[chunk].start
        return pl.ds(pl.multiple_of(start, LANES), plan.chunks[chunk].width)

    def tile_base(base, part):
        return pl.multiple_of(base + (part // splits) * SUBLANES, SUBLANES)

    def tile_rows(chunk, base, part):
        return pl.ds(tile_base(base, part) + plan.chunks[chunk].row, plan.chunks[chunk].rows)

    def own_rows(chunk):
        return by_rows[chunk].at[pl.ds(gx * held, held)]

    def load(chunk):
        state = plan.chunks[chunk].state
        for off in [*range(1, groups_x), 0]:
            part = peers_x[off]
            target = own_rows(chunk) if off == 0 else ready[chunk].at[off - 1]
            piece = olds[state].at[:, tile_rows(chunk, 0, part), columns(chunk, part)]
            pltpu.make_async_copy(piece, target, local_sem.at[0 if chunk < FIRST_LOADS else 1]).start()

    def first_sends(chunk):
        for off in range(1, groups_x):
            pltpu.make_async_remote_copy(
                src_ref=ready[chunk].at[off - 1],
                dst_ref=own_rows(chunk),
                send_sem=sent,
                recv_sem=recv1.at[chunk],
                device_id=(peers_x[off], gy),
                device_id_type=MESH,
            ).start()

    def count_copy(rows, k, sem, px, py):
        return pltpu.make_async_remote_copy(
            src_ref=rows.at[k],
            dst_ref=rows.at[k],
            send_sem=sent,
            recv_sem=recv_c.at[sem],
            device_id=(px, py),
            device_id_type=MESH,
        )

    for chunk in range(FIRST_LOADS):
        load(chunk)
    for copy in small:
        copy.start()
    for chunk in range(FIRST_LOADS, chunks):
        load(chunk)
    grad_copy.start()

    pl.semaphore_wait(barrier, groups_x - 1 + plane * (1 + side) + side)
    for off in range(1, groups_x):
        signal(row_in, peers_x[off], gy)

    for chunk in range(FIRST_LOADS):
        landed(by_rows[chunk], local_sem.at[0])
    for chunk in range(FIRST_LOADS):
        first_sends(chunk)
    for copy in small:
        copy.wait()
    for off in range(1, groups_x):
        count_copy(row_counts, gx, 0, peers_x[off], gy).start()
    for chunk in range(FIRST_LOADS, chunks):
        landed(by_rows[chunk], local_sem.at[1])
    for chunk in range(FIRST_LOADS, chunks):
        first_sends(chunk)

    owners = [new_owner[e] for e in range(experts)]
    places = [old_owner[e] for e in range(experts)]

    def find(slot, carry):
        total = jnp.int32(0)
        for e in range(experts):
            total = total + jnp.where(owners[e] == slot, places[e], 0)
        source[slot] = total
        return carry

    pl.semaphore_wait(row_in, groups_x - 1)

    @pl.when(side == 1)
    def _():
        signal(mate_in, gx, mate)

        @pl.when(has_low)
        def _():
            signal(up_in, gx, gy - PAIR)
            signal(up_in, gx, mate - PAIR)

    lax.fori_loop(0, experts, find, 0)

    pl.when(side == 0)(lambda: pl.semaphore_wait(mate_in, 1))

    def meet_upper():
        pl.semaphore_wait(up_in, 1)
        if planes > 2:
            pl.when(has_low)(lambda: signal(far_up.at[0], gx, gy - PAIR))

    pl.when(upper == 0)(meet_upper)

    def landing(chunk):
        return moved.at[plan.chunks[chunk].state, tile_rows(chunk, gy * rows, gx), columns(chunk, gx)]

    def send(chunk, px, py):
        pltpu.make_async_remote_copy(
            src_ref=staged[chunk].at[px * groups_y + py],
            dst_ref=landing(chunk),
            send_sem=sent,
            recv_sem=recv2.at[plan.chunks[chunk].lands],
            device_id=(px, py),
            device_id_type=MESH,
        ).start()

    def send_counts():
        landed(row_counts.at[pl.ds(0, groups_x - 1)], recv_c.at[0])
        all_counts[gy] = jnp.sum(row_counts[...], axis=0)
        for off in range(1, groups_y):
            count_copy(all_counts, gy, 1, gx, (gy + off) % groups_y).start()

    def to_plane(fn, target):
        for pair in range(PAIR):
            py = target * PAIR + (side + pair + 1) % PAIR
            for px in peers_x[1:] + peers_x[:1]:
                fn(px, py)

    def to_own_plane(fn):
        for px in peers_x:
            fn(px, mate)
        for px in peers_x[1:]:
            fn(px, gy)

    def to_upper(fns, far):
        pl.semaphore_wait(far_up.at[far - 2], 1)
        if far < planes - 1:
            pl.when(has_low)(lambda: signal(far_up.at[far - 1], gx, gy - PAIR))
        for fn in fns:
            to_plane(fn, plane + far)

    def spread(fn):
        for k in range(half):
            to_plane(fn, upper * k + (1 - upper) * (planes - 1 - k))
        for k in range(1, half):
            to_plane(fn, upper * half + (plane + k) % half)
        to_own_plane(fn)

    def stage(chunk):
        landed(ready[chunk], recv1.at[chunk])

        def one(slot, carry):
            staged[chunk][slot] = by_rows[chunk][source[slot]]
            return carry

        lax.fori_loop(0, experts, one, 0, unroll=4)
        if chunk >= FIRST_LOADS:
            landing(chunk)[...] = by_rows[chunk][source[me]]
        elif chunk == FIRST_LOADS - 1:
            own = [by_rows[k][source[me]] for k in range(FIRST_LOADS)]
            moved[TURNS[0], pl.ds(tile_base(gy * rows, gx), SUBLANES), columns(0, gx)] = jnp.concatenate(own)

    opening = {far: FIRST_LOADS + far - 2 for far in range(2, planes)}
    early = opening[planes - 1] + 1
    for chunk in range(early):
        stage(chunk)
        fn = functools.partial(send, chunk)
        pl.when(upper == 0)(functools.partial(to_plane, fn, plane + 1))
        for k in range(1, planes):
            pl.when(plane >= k)(functools.partial(to_plane, fn, plane - k))
        above = jnp.logical_and(upper == 1, has_high)
        if chunk == 0:
            pl.when(above)(meet_upper)
        pl.when(above)(functools.partial(to_plane, fn, plane + 1))
        for far, opens in opening.items():
            if chunk > opens:
                pl.when(plane < planes - far)(functools.partial(to_plane, fn, plane + far))
            if chunk == opens:
                fns = [functools.partial(send, k) for k in range(chunk + 1)]
                pl.when(plane < planes - far)(functools.partial(to_upper, fns, far))
        to_own_plane(fn)

    def step(chunk):
        stage(chunk)
        spread(functools.partial(send, chunk))

    for chunk in range(early, chunks):
        step(chunk)
        if chunk == early:
            send_counts()

    landed(all_counts.at[pl.ds(0, groups_y - 1)], recv_c.at[1])
    grad_copy.wait()
    totals = jnp.sum(all_counts[...].astype(jnp.float32), axis=0)
    slot_count = jnp.sum(jnp.where(owner_row[...] == me, totals, 0.0), axis=1, keepdims=True)
    per_token = 1.0 / slot_count

    def tiles(start, width, fn):
        def one(step, carry):
            row = pl.ds(pl.multiple_of(step * ADAM_ROWS, ADAM_ROWS), ADAM_ROWS)
            for part in range(splits):
                fn(row, pl.ds(part * plan.span + start, width))
            return carry

        lax.fori_loop(0, rows * groups_y // ADAM_ROWS, one, 0, unroll=2)

    def moments(row, col):
        moved[FIRST, row, col], moved[SECOND, row, col], steps[row, col] = adam_direction(
            moved[FIRST, row, col], moved[SECOND, row, col], grad[0, row, col], per_token
        )

    def weights(row, col):
        moved[MASTER, row, col] = adam_weights(moved[MASTER, row, col], steps[row, col])

    def all_landed(group, states, width):
        landed(sizes.at[:, :, pl.ds(0, states * width)], recv2.at[group])

    last_start, last_width = plan.bands[-1]
    all_landed(EARLY_BANDS, STATES, last_start)
    for start, width in plan.bands[:-1]:
        tiles(start, width, moments)
        tiles(start, width, weights)
    all_landed(LAST_MOMENTS, STATES - 1, last_width)
    tiles(last_start, last_width, moments)
    all_landed(LAST_WEIGHTS, 1, last_width)
    tiles(last_start, last_width, weights)

    landed(row_counts.at[pl.ds(0, groups_x - 1)], sent)
    landed(all_counts.at[pl.ds(0, groups_y - 1)], sent)
    for chunk in range(chunks):
        landed(ready[chunk], sent)
        landed(staged[chunk].at[pl.ds(0, devices - 1)], sent)


def publish_kernel(moved, master, first, second, sem):
    rows = master.shape[1] // PUBLISHED
    copies = [
        pltpu.make_async_copy(moved.at[pl.ds(k, 1), pl.ds(part * rows, rows)], out.at[:, pl.ds(part * rows, rows)], sem)
        for k, out in enumerate((master, first, second))
        for part in range(PUBLISHED)
    ]
    for copy in copies:
        copy.start()
    for copy in copies:
        copy.wait()


class Chunk(NamedTuple):
    state: int
    start: int
    width: int
    row: int
    rows: int
    lands: int


class Plan:
    def __init__(self, groups_x, groups_y, shape, experts):
        self.groups_x, self.groups_y, self.experts = groups_x, groups_y, experts
        self.held, self.rows, cols = shape
        self.fits = False
        if self.rows % SUBLANES or experts != groups_x * groups_y or groups_y % (2 * PAIR) or groups_y == 2 * PAIR:
            return
        self.tiles = self.rows // SUBLANES
        if groups_x % self.tiles or self.rows * groups_y % ADAM_ROWS:
            return
        self.span = cols // (groups_x // self.tiles)
        if self.span % LANES or cols % (groups_x // self.tiles):
            return
        blocks = self.span // LANES
        widths = [1, *[BAND] * ((blocks - 1) // BAND), (blocks - 1) % BAND]
        widths = WIDTHS if sum(WIDTHS) == blocks else [width for width in widths if width]
        self.bands = [(LANES * sum(widths[:k]), LANES * width) for k, width in enumerate(widths)]
        self.chunks = []
        for start, width in self.bands:
            for state in TURNS:
                lands = EARLY_BANDS
                if (start, width) == self.bands[-1]:
                    lands = LAST_WEIGHTS if state == MASTER else LAST_MOMENTS
                pieces = FIRST_LOADS if not self.chunks else 1
                for k in range(pieces):
                    size = SUBLANES // pieces
                    self.chunks.append(Chunk(state, start, width, k * size, size, lands))
        self.fits = len(widths) > 1 and len(self.chunks) > FIRST_LOADS + groups_y // PAIR


def kernel_body(plan, old_master, old_first, old_second, new_grad, counts, old_owner, new_owner):
    experts = plan.experts
    devices = plan.groups_x * plan.groups_y
    chunks = len(plan.chunks)
    rows, cols = plan.rows * plan.groups_y, old_master.shape[2]
    vmem = pl.BlockSpec(memory_space=pltpu.VMEM)
    hbm = pl.BlockSpec(memory_space=pltpu.HBM)
    far = max(plan.groups_y // PAIR - 2, 1)
    by_rows = [pltpu.VMEM((experts, chunk.rows, chunk.width), jnp.float32) for chunk in plan.chunks]
    ready = [
        pltpu.VMEM((plan.groups_x - 1, plan.held, chunk.rows, chunk.width), jnp.float32) for chunk in plan.chunks
    ]
    row = new_owner.reshape(1, experts)
    operands = (
        old_owner, new_owner, row, counts.reshape(1, experts), new_grad, old_master, old_first, old_second,
    )
    kept = [pltpu.with_memory_space_constraint(array, pltpu.HBM) for array in operands]
    moved = pl.pallas_call(
        functools.partial(rehome_kernel, plan),
        out_shape=jax.ShapeDtypeStruct((STATES, rows, cols), jnp.float32),
        in_specs=[hbm] * 8,
        out_specs=vmem,
        scratch_shapes=by_rows * 2
        + ready
        + [
            pltpu.SMEM((experts,), jnp.int32),
            pltpu.SMEM((experts,), jnp.int32),
            pltpu.SMEM((experts,), jnp.int32),
            pltpu.VMEM((1, experts), jnp.int32),
            pltpu.VMEM((plan.groups_x, 1, experts), jnp.int32),
            pltpu.VMEM((plan.groups_y, 1, experts), jnp.int32),
            pltpu.VMEM((1, rows, cols), new_grad.dtype),
            pltpu.VMEM((rows, cols), jnp.float32),
            pltpu.VMEM((devices - 1, SUBLANES, STATES * plan.span), jnp.float32),
            pltpu.SemaphoreType.DMA,
            pltpu.SemaphoreType.DMA,
            pltpu.SemaphoreType.DMA((2,)),
            pltpu.SemaphoreType.DMA,
            pltpu.SemaphoreType.DMA((chunks,)),
            pltpu.SemaphoreType.DMA((3,)),
            pltpu.SemaphoreType.DMA((2,)),
            pltpu.SemaphoreType.REGULAR,
            pltpu.SemaphoreType.REGULAR,
            pltpu.SemaphoreType.REGULAR,
            pltpu.SemaphoreType.REGULAR((far,)),
        ],
        compiler_params=pltpu.CompilerParams(collective_id=0, has_side_effects=True, vmem_limit_bytes=VMEM_GRANT),
    )(*kept)
    return pl.pallas_call(
        publish_kernel,
        out_shape=[jax.ShapeDtypeStruct((1, rows, cols), jnp.float32)] * STATES,
        in_specs=[pl.BlockSpec(memory_space=pl.ANY)],
        out_specs=[hbm] * STATES,
        scratch_shapes=[pltpu.SemaphoreType.DMA],
        compiler_params=pltpu.CompilerParams(vmem_limit_bytes=1 << 20),
    )(moved)


def body(old_master, old_first, old_second, new_grad, counts, old_owner, new_owner):
    plan = Plan(lax.axis_size("gx"), lax.axis_size("gy"), old_master.shape, old_owner.shape[0])
    if not plan.fits:
        return plain_body(old_master, old_first, old_second, new_grad, counts, old_owner, new_owner)
    return kernel_body(plan, old_master, old_first, old_second, new_grad, counts, old_owner, new_owner)


def solution(mesh):
    placed = (
        P("gx", "gy", None),
        P("gx", "gy", None),
        P("gx", "gy", None),
        P(("gx", "gy"), None, None),
        P(None, ("gx", "gy")),
        P(),
        P(),
    )
    return jax.shard_map(
        body,
        mesh=mesh,
        in_specs=placed,
        out_specs=(P(("gx", "gy"), None, None),) * 3,
        check_vma=False,
    )
```

```python
import functools
from typing import NamedTuple

import jax
import jax.numpy as jnp
from jax import lax
from jax.experimental import pallas as pl
from jax.experimental.pallas import tpu as pltpu
from jax.sharding import PartitionSpec as P

first_correction = 1.0 - 0.9**10
second_correction = 1.0 - 0.999**10
MESH = pl.DeviceIdType.MESH
LANES = 128
VMEM_GRANT = 24 << 20
SUBLANES = 8
PAIR = 2
CORES = 2
STATES = 3
MASTER, FIRST, SECOND = range(STATES)
TURNS = (FIRST, SECOND, MASTER)
FIRST_LOADS = 2
EARLY_BANDS, LAST_MOMENTS, LAST_WEIGHTS = range(3)
ADAM_ROWS = 16
PUBLISHED = 4
BAND = 2
WIDTHS = (1, 2, 3)


def adam_step(master, first, second, grad, slot_count):
    scaled = grad.astype(jnp.float32) / slot_count
    new_first = 0.9 * first + 0.1 * scaled
    new_second = 0.999 * second + 0.001 * scaled * scaled
    step_dir = new_first / first_correction / (jnp.sqrt(new_second / second_correction) + 1e-08)
    new_master = master - 0.01 * (step_dir + 0.1 * master)
    return (new_master, new_first, new_second)


def adam_direction(first, second, grad, per_token):
    scaled = grad.astype(jnp.float32) * per_token
    new_first = 0.9 * first + 0.1 * scaled
    new_second = 0.999 * second + 0.001 * scaled * scaled
    step_dir = new_first * (1.0 / first_correction) / (jnp.sqrt(new_second * (1.0 / second_correction)) + 1e-08)
    return (new_first, new_second, step_dir)


def adam_weights(master, step_dir):
    return master - 0.01 * (step_dir + 0.1 * master)


def reorder(block, groups_x, groups_y):
    total_rows = block.shape[1]
    piece = total_rows // (groups_x * groups_y)
    shaped = block.reshape(1, groups_x, groups_y, piece, block.shape[2])
    return shaped.transpose(0, 2, 1, 3, 4).reshape(1, total_rows, block.shape[2])


def plain_body(old_master, old_first, old_second, new_grad, counts, old_owner, new_owner):
    experts = old_owner.shape[0]
    groups_x = lax.axis_size("gx")
    groups_y = lax.axis_size("gy")
    my_slot = lax.axis_index("gx") * groups_y + lax.axis_index("gy")
    slots = jnp.arange(experts, dtype=jnp.int32)
    onehot = new_owner[:, None] == slots[None, :]
    source = jnp.sum(jnp.where(onehot, old_owner[:, None], 0), axis=0)
    local_counts = counts[:, 0].astype(jnp.float32)
    by_rows = tuple(
        lax.all_to_all(state, "gx", split_axis=1, concat_axis=0, tiled=True)
        for state in (old_master, old_first, old_second)
    )
    permuted = tuple((jnp.take(state, source, axis=0) for state in by_rows))
    landed = lax.all_to_all(permuted, ("gx", "gy"), split_axis=0, concat_axis=1, tiled=True)
    arrived = tuple((reorder(state, groups_x, groups_y) for state in landed))
    totals = lax.psum(local_counts, ("gx", "gy"))
    slot_count = jnp.sum(jnp.where(new_owner == my_slot, totals, jnp.float32(0.0)))
    return adam_step(arrived[0], arrived[1], arrived[2], new_grad, slot_count)


def rehome_kernel(
    plan, old_owner_hbm, new_owner_hbm, owner_row_hbm, count_row, grad_hbm, old_m, old_f, old_s, moved, *scratch
):
    chunks = len(plan.chunks)
    by_rows, staged, ready = (scratch[k * chunks : (k + 1) * chunks] for k in range(3))
    (
        source, old_owner, new_owner, owner_row, row_counts, all_counts, grad, steps, sizes,
        small_sem, grad_sem, local_sem, sent, recv1, recv2, recv_c,
        row_in, up_in, mate_in, far_up,
    ) = scratch[3 * chunks :]
    olds = (old_m, old_f, old_s)
    groups_x, groups_y, experts, held, rows = plan.groups_x, plan.groups_y, plan.experts, plan.held, plan.rows
    devices = groups_x * groups_y
    splits = groups_x // plan.tiles
    planes = groups_y // PAIR
    half = planes // 2
    gx = lax.axis_index("gx")
    gy = lax.axis_index("gy")
    me = gx * groups_y + gy
    plane = gy // PAIR
    side = gy % PAIR
    mate = gy + 1 - 2 * side
    upper = plane // half
    has_low = plane > 0
    has_high = plane < planes - 1

    core = gx % CORES
    peers_x = [gx]
    for k in range(1, groups_x // CORES):
        peers_x += [(gx - core + CORES * k) % groups_x + CORES - 1 - c for c in range(CORES)]
    peers_x += [gx - core + (core + k) % CORES for k in range(1, CORES)]

    def signal(sem, px, py):
        pl.semaphore_signal(sem, inc=1, device_id=(px, py), device_id_type=MESH)

    barrier = pltpu.get_barrier_semaphore()
    for off in range(1, groups_x):
        signal(barrier, peers_x[off], gy)

    def greet(k):
        signal(barrier, gx, gy + k * PAIR)
        pl.when(side == 0)(lambda: signal(barrier, gx, mate + k * PAIR))

    for k in range(1, planes):
        pl.when(plane + k < planes)(functools.partial(greet, k))

    pl.when(side == 0)(lambda: signal(barrier, gx, mate))

    small = (
        pltpu.make_async_copy(old_owner_hbm, old_owner, small_sem),
        pltpu.make_async_copy(new_owner_hbm, new_owner, small_sem),
        pltpu.make_async_copy(owner_row_hbm, owner_row, small_sem),
        pltpu.make_async_copy(count_row, row_counts.at[gx], small_sem),
    )
    grad_copy = pltpu.make_async_copy(grad_hbm, grad, grad_sem)

    def landed(ref, sem):
        pltpu.make_async_copy(ref, ref, sem).wait()

    def columns(chunk, part):
        start = (part % splits) * plan.span + plan.chunks[chunk].start
        return pl.ds(pl.multiple_of(start, LANES), plan.chunks[chunk].width)

    def tile_base(base, part):
        return pl.multiple_of(base + (part // splits) * SUBLANES, SUBLANES)

    def tile_rows(chunk, base, part):
        return pl.ds(tile_base(base, part) + plan.chunks[chunk].row, plan.chunks[chunk].rows)

    def own_rows(chunk):
        return by_rows[chunk].at[pl.ds(gx * held, held)]

    def load(chunk):
        state = plan.chunks[chunk].state
        for off in [*range(1, groups_x), 0]:
            part = peers_x[off]
            target = own_rows(chunk) if off == 0 else ready[chunk].at[off - 1]
            piece = olds[state].at[:, tile_rows(chunk, 0, part), columns(chunk, part)]
            pltpu.make_async_copy(piece, target, local_sem.at[0 if chunk < FIRST_LOADS else 1]).start()

    def first_sends(chunk):
        for off in range(1, groups_x):
            pltpu.make_async_remote_copy(
                src_ref=ready[chunk].at[off - 1],
                dst_ref=own_rows(chunk),
                send_sem=sent,
                recv_sem=recv1.at[chunk],
                device_id=(peers_x[off], gy),
                device_id_type=MESH,
            ).start()

    def count_copy(rows, k, sem, px, py):
        return pltpu.make_async_remote_copy(
            src_ref=rows.at[k],
            dst_ref=rows.at[k],
            send_sem=sent,
            recv_sem=recv_c.at[sem],
            device_id=(px, py),
            device_id_type=MESH,
        )

    for chunk in range(FIRST_LOADS):
        load(chunk)
    for copy in small:
        copy.start()
    for chunk in range(FIRST_LOADS, chunks):
        load(chunk)
    grad_copy.start()

    pl.semaphore_wait(barrier, groups_x - 1 + plane * (1 + side) + side)
    for off in range(1, groups_x):
        signal(row_in, peers_x[off], gy)

    for chunk in range(FIRST_LOADS):
        landed(by_rows[chunk], local_sem.at[0])
    for chunk in range(FIRST_LOADS):
        first_sends(chunk)
    for copy in small:
        copy.wait()
    for off in range(1, groups_x):
        count_copy(row_counts, gx, 0, peers_x[off], gy).start()
    for chunk in range(FIRST_LOADS, chunks):
        landed(by_rows[chunk], local_sem.at[1])
    for chunk in range(FIRST_LOADS, chunks):
        first_sends(chunk)

    owners = [new_owner[e] for e in range(experts)]
    places = [old_owner[e] for e in range(experts)]

    def find(slot, carry):
        total = jnp.int32(0)
        for e in range(experts):
            total = total + jnp.where(owners[e] == slot, places[e], 0)
        source[slot] = total
        return carry

    pl.semaphore_wait(row_in, groups_x - 1)

    @pl.when(side == 1)
    def _():
        signal(mate_in, gx, mate)

        @pl.when(has_low)
        def _():
            signal(up_in, gx, gy - PAIR)
            signal(up_in, gx, mate - PAIR)

    lax.fori_loop(0, experts, find, 0)

    pl.when(side == 0)(lambda: pl.semaphore_wait(mate_in, 1))

    def meet_upper():
        pl.semaphore_wait(up_in, 1)
        if planes > 2:
            pl.when(has_low)(lambda: signal(far_up.at[0], gx, gy - PAIR))

    pl.when(upper == 0)(meet_upper)

    def landing(chunk):
        return moved.at[plan.chunks[chunk].state, tile_rows(chunk, gy * rows, gx), columns(chunk, gx)]

    def send(chunk, px, py):
        pltpu.make_async_remote_copy(
            src_ref=staged[chunk].at[px * groups_y + py],
            dst_ref=landing(chunk),
            send_sem=sent,
            recv_sem=recv2.at[plan.chunks[chunk].lands],
            device_id=(px, py),
            device_id_type=MESH,
        ).start()

    def send_counts():
        landed(row_counts.at[pl.ds(0, groups_x - 1)], recv_c.at[0])
        all_counts[gy] = jnp.sum(row_counts[...], axis=0)
        for off in range(1, groups_y):
            count_copy(all_counts, gy, 1, gx, (gy + off) % groups_y).start()

    def to_plane(fn, target):
        for pair in range(PAIR):
            py = target * PAIR + (side + pair + 1) % PAIR
            for px in peers_x[1:] + peers_x[:1]:
                fn(px, py)

    def to_own_plane(fn):
        for px in peers_x:
            fn(px, mate)
        for px in peers_x[1:]:
            fn(px, gy)

    def to_upper(fns, far):
        pl.semaphore_wait(far_up.at[far - 2], 1)
        if far < planes - 1:
            pl.when(has_low)(lambda: signal(far_up.at[far - 1], gx, gy - PAIR))
        for fn in fns:
            to_plane(fn, plane + far)

    def spread_last(fn):
        row = CORES
        corner = [(0, px) for px in reversed(range(row))]
        rest = [(pair, px) for px in range(groups_x) for pair in range(PAIR) if (pair, px) not in corner]

        def to_part(target, part):
            for pair, px in part:
                fn(px, target * PAIR + pair)

        def downward():
            for part in (corner, rest):
                for target in range(half):
                    to_part(target, part)

        def upward():
            for part in (corner, rest):
                for target in range(half, planes):
                    to_part(target, part)

        pl.when(upper == 1)(downward)
        pl.when(upper == 0)(upward)
        for k in range(1, half):
            to_plane(fn, upper * half + (plane + k) % half)
        to_own_plane(fn)

    def spread(fn):
        for k in range(half):
            to_plane(fn, upper * k + (1 - upper) * (planes - 1 - k))
        for k in range(1, half):
            to_plane(fn, upper * half + (plane + k) % half)
        to_own_plane(fn)

    def stage(chunk):
        landed(ready[chunk], recv1.at[chunk])

        def one(slot, carry):
            staged[chunk][slot] = by_rows[chunk][source[slot]]
            return carry

        lax.fori_loop(0, experts, one, 0, unroll=4)
        if chunk >= FIRST_LOADS:
            landing(chunk)[...] = by_rows[chunk][source[me]]
        elif chunk == FIRST_LOADS - 1:
            own = [by_rows[k][source[me]] for k in range(FIRST_LOADS)]
            moved[TURNS[0], pl.ds(tile_base(gy * rows, gx), SUBLANES), columns(0, gx)] = jnp.concatenate(own)

    opening = {far: FIRST_LOADS + far - 2 for far in range(2, planes)}
    early = opening[planes - 1] + 1
    for chunk in range(early):
        stage(chunk)
        fn = functools.partial(send, chunk)
        pl.when(upper == 0)(functools.partial(to_plane, fn, plane + 1))
        for k in range(1, planes):
            pl.when(plane >= k)(functools.partial(to_plane, fn, plane - k))
        above = jnp.logical_and(upper == 1, has_high)
        if chunk == 0:
            pl.when(above)(meet_upper)
        pl.when(above)(functools.partial(to_plane, fn, plane + 1))
        for far, opens in opening.items():
            if chunk > opens:
                pl.when(plane < planes - far)(functools.partial(to_plane, fn, plane + far))
            if chunk == opens:
                fns = [functools.partial(send, k) for k in range(chunk + 1)]
                pl.when(plane < planes - far)(functools.partial(to_upper, fns, far))
        to_own_plane(fn)

    def step(chunk):
        stage(chunk)
        (spread_last if chunk == chunks - 1 else spread)(functools.partial(send, chunk))

    for chunk in range(early, chunks):
        step(chunk)
        if chunk == early:
            send_counts()

    landed(all_counts.at[pl.ds(0, groups_y - 1)], recv_c.at[1])
    grad_copy.wait()
    totals = jnp.sum(all_counts[...].astype(jnp.float32), axis=0)
    slot_count = jnp.sum(jnp.where(owner_row[...] == me, totals, 0.0), axis=1, keepdims=True)
    per_token = 1.0 / slot_count

    def tiles(start, width, fn):
        def one(step, carry):
            row = pl.ds(pl.multiple_of(step * ADAM_ROWS, ADAM_ROWS), ADAM_ROWS)
            for part in range(splits):
                fn(row, pl.ds(part * plan.span + start, width))
            return carry

        lax.fori_loop(0, rows * groups_y // ADAM_ROWS, one, 0, unroll=2)

    def moments(row, col):
        moved[FIRST, row, col], moved[SECOND, row, col], steps[row, col] = adam_direction(
            moved[FIRST, row, col], moved[SECOND, row, col], grad[0, row, col], per_token
        )

    def weights(row, col):
        moved[MASTER, row, col] = adam_weights(moved[MASTER, row, col], steps[row, col])

    def all_landed(group, states, width):
        landed(sizes.at[:, :, pl.ds(0, states * width)], recv2.at[group])

    last_start, last_width = plan.bands[-1]
    all_landed(EARLY_BANDS, STATES, last_start)
    for start, width in plan.bands[:-1]:
        tiles(start, width, moments)
        tiles(start, width, weights)
    all_landed(LAST_MOMENTS, STATES - 1, last_width)
    tiles(last_start, last_width, moments)
    all_landed(LAST_WEIGHTS, 1, last_width)
    tiles(last_start, last_width, weights)

    landed(row_counts.at[pl.ds(0, groups_x - 1)], sent)
    landed(all_counts.at[pl.ds(0, groups_y - 1)], sent)
    for chunk in range(chunks):
        landed(ready[chunk], sent)
        landed(staged[chunk].at[pl.ds(0, devices - 1)], sent)


def publish_kernel(moved, master, first, second, sem):
    rows = master.shape[1] // PUBLISHED
    copies = [
        pltpu.make_async_copy(moved.at[pl.ds(k, 1), pl.ds(part * rows, rows)], out.at[:, pl.ds(part * rows, rows)], sem)
        for k, out in enumerate((master, first, second))
        for part in range(PUBLISHED)
    ]
    for copy in copies:
        copy.start()
    for copy in copies:
        copy.wait()


class Chunk(NamedTuple):
    state: int
    start: int
    width: int
    row: int
    rows: int
    lands: int


class Plan:
    def __init__(self, groups_x, groups_y, shape, experts):
        self.groups_x, self.groups_y, self.experts = groups_x, groups_y, experts
        self.held, self.rows, cols = shape
        self.fits = False
        if self.rows % SUBLANES or experts != groups_x * groups_y or groups_x % CORES or groups_y % (2 * PAIR) or groups_y == 2 * PAIR:
            return
        self.tiles = self.rows // SUBLANES
        if groups_x % self.tiles or self.rows * groups_y % ADAM_ROWS:
            return
        self.span = cols // (groups_x // self.tiles)
        if self.span % LANES or cols % (groups_x // self.tiles):
            return
        blocks = self.span // LANES
        widths = [1, *[BAND] * ((blocks - 1) // BAND), (blocks - 1) % BAND]
        widths = WIDTHS if sum(WIDTHS) == blocks else [width for width in widths if width]
        self.bands = [(LANES * sum(widths[:k]), LANES * width) for k, width in enumerate(widths)]
        self.chunks = []
        for start, width in self.bands:
            for state in TURNS:
                lands = EARLY_BANDS
                if (start, width) == self.bands[-1]:
                    lands = LAST_WEIGHTS if state == MASTER else LAST_MOMENTS
                pieces = FIRST_LOADS if not self.chunks else 1
                for k in range(pieces):
                    size = SUBLANES // pieces
                    self.chunks.append(Chunk(state, start, width, k * size, size, lands))
        self.fits = len(widths) > 1 and len(self.chunks) > FIRST_LOADS + groups_y // PAIR


def kernel_body(plan, old_master, old_first, old_second, new_grad, counts, old_owner, new_owner):
    experts = plan.experts
    devices = plan.groups_x * plan.groups_y
    chunks = len(plan.chunks)
    rows, cols = plan.rows * plan.groups_y, old_master.shape[2]
    vmem = pl.BlockSpec(memory_space=pltpu.VMEM)
    hbm = pl.BlockSpec(memory_space=pltpu.HBM)
    far = max(plan.groups_y // PAIR - 2, 1)
    by_rows = [pltpu.VMEM((experts, chunk.rows, chunk.width), jnp.float32) for chunk in plan.chunks]
    ready = [
        pltpu.VMEM((plan.groups_x - 1, plan.held, chunk.rows, chunk.width), jnp.float32) for chunk in plan.chunks
    ]
    row = new_owner.reshape(1, experts)
    operands = (
        old_owner, new_owner, row, counts.reshape(1, experts), new_grad, old_master, old_first, old_second,
    )
    kept = [pltpu.with_memory_space_constraint(array, pltpu.HBM) for array in operands]
    moved = pl.pallas_call(
        functools.partial(rehome_kernel, plan),
        out_shape=jax.ShapeDtypeStruct((STATES, rows, cols), jnp.float32),
        in_specs=[hbm] * 8,
        out_specs=vmem,
        scratch_shapes=by_rows * 2
        + ready
        + [
            pltpu.SMEM((experts,), jnp.int32),
            pltpu.SMEM((experts,), jnp.int32),
            pltpu.SMEM((experts,), jnp.int32),
            pltpu.VMEM((1, experts), jnp.int32),
            pltpu.VMEM((plan.groups_x, 1, experts), jnp.int32),
            pltpu.VMEM((plan.groups_y, 1, experts), jnp.int32),
            pltpu.VMEM((1, rows, cols), new_grad.dtype),
            pltpu.VMEM((rows, cols), jnp.float32),
            pltpu.VMEM((devices - 1, SUBLANES, STATES * plan.span), jnp.float32),
            pltpu.SemaphoreType.DMA,
            pltpu.SemaphoreType.DMA,
            pltpu.SemaphoreType.DMA((2,)),
            pltpu.SemaphoreType.DMA,
            pltpu.SemaphoreType.DMA((chunks,)),
            pltpu.SemaphoreType.DMA((3,)),
            pltpu.SemaphoreType.DMA((2,)),
            pltpu.SemaphoreType.REGULAR,
            pltpu.SemaphoreType.REGULAR,
            pltpu.SemaphoreType.REGULAR,
            pltpu.SemaphoreType.REGULAR((far,)),
        ],
        compiler_params=pltpu.CompilerParams(collective_id=0, has_side_effects=True, vmem_limit_bytes=VMEM_GRANT),
    )(*kept)
    return pl.pallas_call(
        publish_kernel,
        out_shape=[jax.ShapeDtypeStruct((1, rows, cols), jnp.float32)] * STATES,
        in_specs=[pl.BlockSpec(memory_space=pl.ANY)],
        out_specs=[hbm] * STATES,
        scratch_shapes=[pltpu.SemaphoreType.DMA],
        compiler_params=pltpu.CompilerParams(vmem_limit_bytes=1 << 20),
    )(moved)


def body(old_master, old_first, old_second, new_grad, counts, old_owner, new_owner):
    plan = Plan(lax.axis_size("gx"), lax.axis_size("gy"), old_master.shape, old_owner.shape[0])
    if not plan.fits:
        return plain_body(old_master, old_first, old_second, new_grad, counts, old_owner, new_owner)
    return kernel_body(plan, old_master, old_first, old_second, new_grad, counts, old_owner, new_owner)


def solution(mesh):
    placed = (
        P("gx", "gy", None),
        P("gx", "gy", None),
        P("gx", "gy", None),
        P(("gx", "gy"), None, None),
        P(None, ("gx", "gy")),
        P(),
        P(),
    )
    return jax.shard_map(
        body,
        mesh=mesh,
        in_specs=placed,
        out_specs=(P(("gx", "gy"), None, None),) * 3,
        check_vma=False,
    )
```

```python
import functools
from typing import NamedTuple

import jax
import jax.numpy as jnp
from jax import lax
from jax.experimental import pallas as pl
from jax.experimental.pallas import tpu as pltpu
from jax.sharding import PartitionSpec as P

first_correction = 1.0 - 0.9**10
second_correction = 1.0 - 0.999**10
MESH = pl.DeviceIdType.MESH
LANES = 128
VMEM_GRANT = 24 << 20
SUBLANES = 8
PAIR = 2
CORES = 2
STATES = 3
MASTER, FIRST, SECOND = range(STATES)
TURNS = (FIRST, SECOND, MASTER)
FIRST_LOADS = 4
EARLY_BANDS, LAST_MOMENTS, LAST_WEIGHTS = range(3)
ADAM_ROWS = 16
PUBLISHED = 4
BAND = 2
WIDTHS = (1, 2, 3)


def adam_step(master, first, second, grad, slot_count):
    scaled = grad.astype(jnp.float32) / slot_count
    new_first = 0.9 * first + 0.1 * scaled
    new_second = 0.999 * second + 0.001 * scaled * scaled
    step_dir = new_first / first_correction / (jnp.sqrt(new_second / second_correction) + 1e-08)
    new_master = master - 0.01 * (step_dir + 0.1 * master)
    return (new_master, new_first, new_second)


def adam_direction(first, second, grad, per_token):
    scaled = grad.astype(jnp.float32) * per_token
    new_first = 0.9 * first + 0.1 * scaled
    new_second = 0.999 * second + 0.001 * scaled * scaled
    step_dir = new_first * (1.0 / first_correction) / (jnp.sqrt(new_second * (1.0 / second_correction)) + 1e-08)
    return (new_first, new_second, step_dir)


def adam_weights(master, step_dir):
    return master - 0.01 * (step_dir + 0.1 * master)


def reorder(block, groups_x, groups_y):
    total_rows = block.shape[1]
    piece = total_rows // (groups_x * groups_y)
    shaped = block.reshape(1, groups_x, groups_y, piece, block.shape[2])
    return shaped.transpose(0, 2, 1, 3, 4).reshape(1, total_rows, block.shape[2])


def plain_body(old_master, old_first, old_second, new_grad, counts, old_owner, new_owner):
    experts = old_owner.shape[0]
    groups_x = lax.axis_size("gx")
    groups_y = lax.axis_size("gy")
    my_slot = lax.axis_index("gx") * groups_y + lax.axis_index("gy")
    slots = jnp.arange(experts, dtype=jnp.int32)
    onehot = new_owner[:, None] == slots[None, :]
    source = jnp.sum(jnp.where(onehot, old_owner[:, None], 0), axis=0)
    local_counts = counts[:, 0].astype(jnp.float32)
    by_rows = tuple(
        lax.all_to_all(state, "gx", split_axis=1, concat_axis=0, tiled=True)
        for state in (old_master, old_first, old_second)
    )
    permuted = tuple((jnp.take(state, source, axis=0) for state in by_rows))
    landed = lax.all_to_all(permuted, ("gx", "gy"), split_axis=0, concat_axis=1, tiled=True)
    arrived = tuple((reorder(state, groups_x, groups_y) for state in landed))
    totals = lax.psum(local_counts, ("gx", "gy"))
    slot_count = jnp.sum(jnp.where(new_owner == my_slot, totals, jnp.float32(0.0)))
    return adam_step(arrived[0], arrived[1], arrived[2], new_grad, slot_count)


def rehome_kernel(
    plan, old_owner_hbm, new_owner_hbm, owner_row_hbm, count_row, grad_hbm, old_m, old_f, old_s, moved, *scratch
):
    chunks = len(plan.chunks)
    by_rows, staged, ready = (scratch[k * chunks : (k + 1) * chunks] for k in range(3))
    (
        source, old_owner, new_owner, owner_row, row_counts, all_counts, grad, steps, sizes,
        small_sem, grad_sem, local_sem, sent, recv1, recv2, recv_c,
        row_in, up_in, mate_in, far_up,
    ) = scratch[3 * chunks :]
    olds = (old_m, old_f, old_s)
    groups_x, groups_y, experts, held, rows = plan.groups_x, plan.groups_y, plan.experts, plan.held, plan.rows
    devices = groups_x * groups_y
    splits = groups_x // plan.tiles
    planes = groups_y // PAIR
    half = planes // 2
    gx = lax.axis_index("gx")
    gy = lax.axis_index("gy")
    me = gx * groups_y + gy
    plane = gy // PAIR
    side = gy % PAIR
    mate = gy + 1 - 2 * side
    upper = plane // half
    has_low = plane > 0
    has_high = plane < planes - 1

    core = gx % CORES
    peers_x = [gx]
    for k in range(1, groups_x // CORES):
        peers_x += [(gx - core + CORES * k) % groups_x + CORES - 1 - c for c in range(CORES)]
    peers_x += [gx - core + (core + k) % CORES for k in range(1, CORES)]

    def signal(sem, px, py):
        pl.semaphore_signal(sem, inc=1, device_id=(px, py), device_id_type=MESH)

    barrier = pltpu.get_barrier_semaphore()
    for off in range(1, groups_x):
        signal(barrier, peers_x[off], gy)

    def greet(k):
        signal(barrier, gx, gy + k * PAIR)
        pl.when(side == 0)(lambda: signal(barrier, gx, mate + k * PAIR))

    for k in range(1, planes):
        pl.when(plane + k < planes)(functools.partial(greet, k))

    pl.when(side == 0)(lambda: signal(barrier, gx, mate))

    small = (
        pltpu.make_async_copy(old_owner_hbm, old_owner, small_sem),
        pltpu.make_async_copy(new_owner_hbm, new_owner, small_sem),
        pltpu.make_async_copy(owner_row_hbm, owner_row, small_sem),
        pltpu.make_async_copy(count_row, row_counts.at[gx], small_sem),
    )
    grad_copy = pltpu.make_async_copy(grad_hbm, grad, grad_sem)

    def landed(ref, sem):
        pltpu.make_async_copy(ref, ref, sem).wait()

    def columns(chunk, part):
        start = (part % splits) * plan.span + plan.chunks[chunk].start
        return pl.ds(pl.multiple_of(start, LANES), plan.chunks[chunk].width)

    def tile_base(base, part):
        return pl.multiple_of(base + (part // splits) * SUBLANES, SUBLANES)

    def tile_rows(chunk, base, part):
        return pl.ds(tile_base(base, part) + plan.chunks[chunk].row, plan.chunks[chunk].rows)

    def own_rows(chunk):
        return by_rows[chunk].at[pl.ds(gx * held, held)]

    def load(chunk):
        state = plan.chunks[chunk].state
        for off in [*range(1, groups_x), 0]:
            part = peers_x[off]
            target = own_rows(chunk) if off == 0 else ready[chunk].at[off - 1]
            piece = olds[state].at[:, tile_rows(chunk, 0, part), columns(chunk, part)]
            pltpu.make_async_copy(piece, target, local_sem.at[0 if chunk < FIRST_LOADS else 1]).start()

    def first_sends(chunk):
        for off in range(1, groups_x):
            pltpu.make_async_remote_copy(
                src_ref=ready[chunk].at[off - 1],
                dst_ref=own_rows(chunk),
                send_sem=sent,
                recv_sem=recv1.at[chunk],
                device_id=(peers_x[off], gy),
                device_id_type=MESH,
            ).start()

    def count_copy(rows, k, sem, px, py):
        return pltpu.make_async_remote_copy(
            src_ref=rows.at[k],
            dst_ref=rows.at[k],
            send_sem=sent,
            recv_sem=recv_c.at[sem],
            device_id=(px, py),
            device_id_type=MESH,
        )

    for chunk in range(FIRST_LOADS):
        load(chunk)
    for copy in small:
        copy.start()
    for chunk in range(FIRST_LOADS, chunks):
        load(chunk)
    grad_copy.start()

    pl.semaphore_wait(barrier, groups_x - 1 + plane * (1 + side) + side)
    for off in range(1, groups_x):
        signal(row_in, peers_x[off], gy)

    for chunk in range(FIRST_LOADS):
        landed(by_rows[chunk], local_sem.at[0])
    for chunk in range(FIRST_LOADS):
        first_sends(chunk)
    for copy in small:
        copy.wait()
    for off in range(1, groups_x):
        count_copy(row_counts, gx, 0, peers_x[off], gy).start()
    for chunk in range(FIRST_LOADS, chunks):
        landed(by_rows[chunk], local_sem.at[1])
    for chunk in range(FIRST_LOADS, chunks):
        first_sends(chunk)

    owners = [new_owner[e] for e in range(experts)]
    places = [old_owner[e] for e in range(experts)]

    def find(slot, carry):
        total = jnp.int32(0)
        for e in range(experts):
            total = total + jnp.where(owners[e] == slot, places[e], 0)
        source[slot] = total
        return carry

    pl.semaphore_wait(row_in, groups_x - 1)

    @pl.when(side == 1)
    def _():
        signal(mate_in, gx, mate)

        @pl.when(has_low)
        def _():
            signal(up_in, gx, gy - PAIR)
            signal(up_in, gx, mate - PAIR)

    lax.fori_loop(0, experts, find, 0)

    pl.when(side == 0)(lambda: pl.semaphore_wait(mate_in, 1))

    def meet_upper():
        pl.semaphore_wait(up_in, 1)
        if planes > 2:
            pl.when(has_low)(lambda: signal(far_up.at[0], gx, gy - PAIR))

    pl.when(upper == 0)(meet_upper)

    def landing(chunk):
        return moved.at[plan.chunks[chunk].state, tile_rows(chunk, gy * rows, gx), columns(chunk, gx)]

    def send(chunk, px, py):
        pltpu.make_async_remote_copy(
            src_ref=staged[chunk].at[px * groups_y + py],
            dst_ref=landing(chunk),
            send_sem=sent,
            recv_sem=recv2.at[plan.chunks[chunk].lands],
            device_id=(px, py),
            device_id_type=MESH,
        ).start()

    def send_counts():
        landed(row_counts.at[pl.ds(0, groups_x - 1)], recv_c.at[0])
        all_counts[gy] = jnp.sum(row_counts[...], axis=0)
        for off in range(1, groups_y):
            count_copy(all_counts, gy, 1, gx, (gy + off) % groups_y).start()

    def to_plane(fn, target):
        for pair in range(PAIR):
            py = target * PAIR + (side + pair + 1) % PAIR
            for px in peers_x[1:] + peers_x[:1]:
                fn(px, py)

    def to_own_plane(fn):
        for px in peers_x:
            fn(px, mate)
        for px in peers_x[1:]:
            fn(px, gy)

    def to_upper(fns, far):
        pl.semaphore_wait(far_up.at[far - 2], 1)
        if far < planes - 1:
            pl.when(has_low)(lambda: signal(far_up.at[far - 1], gx, gy - PAIR))
        for fn in fns:
            to_plane(fn, plane + far)

    def spread_last(fn):
        row = CORES
        corner = [(0, px) for px in reversed(range(row))]
        rest = [(pair, px) for pair in range(PAIR) for px in range(groups_x) if (pair, px) not in corner]

        def to_part(target, part):
            for pair, px in part:
                fn(px, target * PAIR + pair)

        def downward():
            for part in (corner, rest):
                for target in range(half):
                    to_part(target, part)

        def upward():
            for part in (corner, rest):
                for target in range(half, planes):
                    to_part(target, part)

        pl.when(upper == 1)(downward)
        pl.when(upper == 0)(upward)
        for k in range(1, half):
            to_plane(fn, upper * half + (plane + k) % half)
        to_own_plane(fn)

    def spread(fn):
        for k in range(half):
            to_plane(fn, upper * k + (1 - upper) * (planes - 1 - k))
        for k in range(1, half):
            to_plane(fn, upper * half + (plane + k) % half)
        to_own_plane(fn)

    def stage(chunk):
        landed(ready[chunk], recv1.at[chunk])

        def one(slot, carry):
            staged[chunk][slot] = by_rows[chunk][source[slot]]
            return carry

        lax.fori_loop(0, experts, one, 0, unroll=4)
        if chunk >= FIRST_LOADS:
            landing(chunk)[...] = by_rows[chunk][source[me]]
        elif chunk == FIRST_LOADS - 1:
            own = [by_rows[k][source[me]] for k in range(FIRST_LOADS)]
            moved[TURNS[0], pl.ds(tile_base(gy * rows, gx), SUBLANES), columns(0, gx)] = jnp.concatenate(own)

    opening = {far: FIRST_LOADS + far - 2 for far in range(2, planes)}
    early = opening[planes - 1] + 1
    for chunk in range(early):
        stage(chunk)
        fn = functools.partial(send, chunk)
        pl.when(upper == 0)(functools.partial(to_plane, fn, plane + 1))
        for k in range(1, planes):
            pl.when(plane >= k)(functools.partial(to_plane, fn, plane - k))
        above = jnp.logical_and(upper == 1, has_high)
        if chunk == 0:
            pl.when(above)(meet_upper)
        pl.when(above)(functools.partial(to_plane, fn, plane + 1))
        for far, opens in opening.items():
            if chunk > opens:
                pl.when(plane < planes - far)(functools.partial(to_plane, fn, plane + far))
            if chunk == opens:
                fns = [functools.partial(send, k) for k in range(chunk + 1)]
                pl.when(plane < planes - far)(functools.partial(to_upper, fns, far))
        to_own_plane(fn)

    def step(chunk):
        stage(chunk)
        (spread_last if chunk == chunks - 1 else spread)(functools.partial(send, chunk))

    for chunk in range(early, chunks):
        step(chunk)
        if chunk == early:
            send_counts()

    landed(all_counts.at[pl.ds(0, groups_y - 1)], recv_c.at[1])
    grad_copy.wait()
    totals = jnp.sum(all_counts[...].astype(jnp.float32), axis=0)
    slot_count = jnp.sum(jnp.where(owner_row[...] == me, totals, 0.0), axis=1, keepdims=True)
    per_token = 1.0 / slot_count

    def tiles(start, width, fn):
        def one(step, carry):
            row = pl.ds(pl.multiple_of(step * ADAM_ROWS, ADAM_ROWS), ADAM_ROWS)
            for part in range(splits):
                fn(row, pl.ds(part * plan.span + start, width))
            return carry

        lax.fori_loop(0, rows * groups_y // ADAM_ROWS, one, 0, unroll=2)

    def moments(row, col):
        moved[FIRST, row, col], moved[SECOND, row, col], steps[row, col] = adam_direction(
            moved[FIRST, row, col], moved[SECOND, row, col], grad[0, row, col], per_token
        )

    def weights(row, col):
        moved[MASTER, row, col] = adam_weights(moved[MASTER, row, col], steps[row, col])

    def all_landed(group, states, width):
        landed(sizes.at[:, :, pl.ds(0, states * width)], recv2.at[group])

    last_start, last_width = plan.bands[-1]
    all_landed(EARLY_BANDS, STATES, last_start)
    for start, width in plan.bands[:-1]:
        tiles(start, width, moments)
        tiles(start, width, weights)
    all_landed(LAST_MOMENTS, STATES - 1, last_width)
    tiles(last_start, last_width, moments)
    all_landed(LAST_WEIGHTS, 1, last_width)
    tiles(last_start, last_width, weights)

    landed(row_counts.at[pl.ds(0, groups_x - 1)], sent)
    landed(all_counts.at[pl.ds(0, groups_y - 1)], sent)
    for chunk in range(chunks):
        landed(ready[chunk], sent)
        landed(staged[chunk].at[pl.ds(0, devices - 1)], sent)


def publish_kernel(moved, master, first, second, sem):
    rows = master.shape[1] // PUBLISHED
    copies = [
        pltpu.make_async_copy(moved.at[pl.ds(k, 1), pl.ds(part * rows, rows)], out.at[:, pl.ds(part * rows, rows)], sem)
        for k, out in enumerate((master, first, second))
        for part in range(PUBLISHED)
    ]
    for copy in copies:
        copy.start()
    for copy in copies:
        copy.wait()


class Chunk(NamedTuple):
    state: int
    start: int
    width: int
    row: int
    rows: int
    lands: int


class Plan:
    def __init__(self, groups_x, groups_y, shape, experts):
        self.groups_x, self.groups_y, self.experts = groups_x, groups_y, experts
        self.held, self.rows, cols = shape
        self.fits = False
        if self.rows % SUBLANES or experts != groups_x * groups_y or groups_x % CORES or groups_y % (2 * PAIR) or groups_y == 2 * PAIR:
            return
        self.tiles = self.rows // SUBLANES
        if groups_x % self.tiles or self.rows * groups_y % ADAM_ROWS:
            return
        self.span = cols // (groups_x // self.tiles)
        if self.span % LANES or cols % (groups_x // self.tiles):
            return
        blocks = self.span // LANES
        widths = [1, *[BAND] * ((blocks - 1) // BAND), (blocks - 1) % BAND]
        widths = WIDTHS if sum(WIDTHS) == blocks else [width for width in widths if width]
        self.bands = [(LANES * sum(widths[:k]), LANES * width) for k, width in enumerate(widths)]
        self.chunks = []
        for start, width in self.bands:
            for state in TURNS:
                lands = EARLY_BANDS
                if (start, width) == self.bands[-1]:
                    lands = LAST_WEIGHTS if state == MASTER else LAST_MOMENTS
                pieces = FIRST_LOADS if not self.chunks else 1
                for k in range(pieces):
                    size = SUBLANES // pieces
                    self.chunks.append(Chunk(state, start, width, k * size, size, lands))
        self.fits = len(widths) > 1 and len(self.chunks) > FIRST_LOADS + groups_y // PAIR


def kernel_body(plan, old_master, old_first, old_second, new_grad, counts, old_owner, new_owner):
    experts = plan.experts
    devices = plan.groups_x * plan.groups_y
    chunks = len(plan.chunks)
    rows, cols = plan.rows * plan.groups_y, old_master.shape[2]
    vmem = pl.BlockSpec(memory_space=pltpu.VMEM)
    hbm = pl.BlockSpec(memory_space=pltpu.HBM)
    far = max(plan.groups_y // PAIR - 2, 1)
    by_rows = [pltpu.VMEM((experts, chunk.rows, chunk.width), jnp.float32) for chunk in plan.chunks]
    ready = [
        pltpu.VMEM((plan.groups_x - 1, plan.held, chunk.rows, chunk.width), jnp.float32) for chunk in plan.chunks
    ]
    row = new_owner.reshape(1, experts)
    operands = (
        old_owner, new_owner, row, counts.reshape(1, experts), new_grad, old_master, old_first, old_second,
    )
    kept = [pltpu.with_memory_space_constraint(array, pltpu.HBM) for array in operands]
    moved = pl.pallas_call(
        functools.partial(rehome_kernel, plan),
        out_shape=jax.ShapeDtypeStruct((STATES, rows, cols), jnp.float32),
        in_specs=[hbm] * 8,
        out_specs=vmem,
        scratch_shapes=by_rows * 2
        + ready
        + [
            pltpu.SMEM((experts,), jnp.int32),
            pltpu.SMEM((experts,), jnp.int32),
            pltpu.SMEM((experts,), jnp.int32),
            pltpu.VMEM((1, experts), jnp.int32),
            pltpu.VMEM((plan.groups_x, 1, experts), jnp.int32),
            pltpu.VMEM((plan.groups_y, 1, experts), jnp.int32),
            pltpu.VMEM((1, rows, cols), new_grad.dtype),
            pltpu.VMEM((rows, cols), jnp.float32),
            pltpu.VMEM((devices - 1, SUBLANES, STATES * plan.span), jnp.float32),
            pltpu.SemaphoreType.DMA,
            pltpu.SemaphoreType.DMA,
            pltpu.SemaphoreType.DMA((2,)),
            pltpu.SemaphoreType.DMA,
            pltpu.SemaphoreType.DMA((chunks,)),
            pltpu.SemaphoreType.DMA((3,)),
            pltpu.SemaphoreType.DMA((2,)),
            pltpu.SemaphoreType.REGULAR,
            pltpu.SemaphoreType.REGULAR,
            pltpu.SemaphoreType.REGULAR,
            pltpu.SemaphoreType.REGULAR((far,)),
        ],
        compiler_params=pltpu.CompilerParams(collective_id=0, has_side_effects=True, vmem_limit_bytes=VMEM_GRANT),
    )(*kept)
    return pl.pallas_call(
        publish_kernel,
        out_shape=[jax.ShapeDtypeStruct((1, rows, cols), jnp.float32)] * STATES,
        in_specs=[pl.BlockSpec(memory_space=pl.ANY)],
        out_specs=[hbm] * STATES,
        scratch_shapes=[pltpu.SemaphoreType.DMA],
        compiler_params=pltpu.CompilerParams(vmem_limit_bytes=1 << 20),
    )(moved)


def body(old_master, old_first, old_second, new_grad, counts, old_owner, new_owner):
    plan = Plan(lax.axis_size("gx"), lax.axis_size("gy"), old_master.shape, old_owner.shape[0])
    if not plan.fits:
        return plain_body(old_master, old_first, old_second, new_grad, counts, old_owner, new_owner)
    return kernel_body(plan, old_master, old_first, old_second, new_grad, counts, old_owner, new_owner)


def solution(mesh):
    placed = (
        P("gx", "gy", None),
        P("gx", "gy", None),
        P("gx", "gy", None),
        P(("gx", "gy"), None, None),
        P(None, ("gx", "gy")),
        P(),
        P(),
    )
    return jax.shard_map(
        body,
        mesh=mesh,
        in_specs=placed,
        out_specs=(P(("gx", "gy"), None, None),) * 3,
        check_vma=False,
    )
```

```python
import functools
from typing import NamedTuple

import jax
import jax.numpy as jnp
from jax import lax
from jax.experimental import pallas as pl
from jax.experimental.pallas import tpu as pltpu
from jax.sharding import PartitionSpec as P

first_correction = 1.0 - 0.9**10
second_correction = 1.0 - 0.999**10
MESH = pl.DeviceIdType.MESH
LANES = 128
VMEM_GRANT = 24 << 20
SUBLANES = 8
PAIR = 2
CORES = 2
STATES = 3
MASTER, FIRST, SECOND = range(STATES)
TURNS = (FIRST, SECOND, MASTER)
FIRST_LOADS = 4
EARLY_BANDS, LAST_MOMENTS, LAST_WEIGHTS = range(3)
ADAM_ROWS = 16
PUBLISHED = 4
BAND = 2
WIDTHS = (1, 2, 3)


def adam_step(master, first, second, grad, slot_count):
    scaled = grad.astype(jnp.float32) / slot_count
    new_first = 0.9 * first + 0.1 * scaled
    new_second = 0.999 * second + 0.001 * scaled * scaled
    step_dir = new_first / first_correction / (jnp.sqrt(new_second / second_correction) + 1e-08)
    new_master = master - 0.01 * (step_dir + 0.1 * master)
    return (new_master, new_first, new_second)


def adam_direction(first, second, grad, per_token):
    scaled = grad.astype(jnp.float32) * per_token
    new_first = 0.9 * first + 0.1 * scaled
    new_second = 0.999 * second + 0.001 * scaled * scaled
    step_dir = new_first * (1.0 / first_correction) / (jnp.sqrt(new_second * (1.0 / second_correction)) + 1e-08)
    return (new_first, new_second, step_dir)


def adam_weights(master, step_dir):
    return master - 0.01 * (step_dir + 0.1 * master)


def reorder(block, groups_x, groups_y):
    total_rows = block.shape[1]
    piece = total_rows // (groups_x * groups_y)
    shaped = block.reshape(1, groups_x, groups_y, piece, block.shape[2])
    return shaped.transpose(0, 2, 1, 3, 4).reshape(1, total_rows, block.shape[2])


def plain_body(old_master, old_first, old_second, new_grad, counts, old_owner, new_owner):
    experts = old_owner.shape[0]
    groups_x = lax.axis_size("gx")
    groups_y = lax.axis_size("gy")
    my_slot = lax.axis_index("gx") * groups_y + lax.axis_index("gy")
    slots = jnp.arange(experts, dtype=jnp.int32)
    onehot = new_owner[:, None] == slots[None, :]
    source = jnp.sum(jnp.where(onehot, old_owner[:, None], 0), axis=0)
    local_counts = counts[:, 0].astype(jnp.float32)
    by_rows = tuple(
        lax.all_to_all(state, "gx", split_axis=1, concat_axis=0, tiled=True)
        for state in (old_master, old_first, old_second)
    )
    permuted = tuple((jnp.take(state, source, axis=0) for state in by_rows))
    landed = lax.all_to_all(permuted, ("gx", "gy"), split_axis=0, concat_axis=1, tiled=True)
    arrived = tuple((reorder(state, groups_x, groups_y) for state in landed))
    totals = lax.psum(local_counts, ("gx", "gy"))
    slot_count = jnp.sum(jnp.where(new_owner == my_slot, totals, jnp.float32(0.0)))
    return adam_step(arrived[0], arrived[1], arrived[2], new_grad, slot_count)


def rehome_kernel(
    plan, old_owner_hbm, new_owner_hbm, owner_row_hbm, count_row, grad_hbm, old_m, old_f, old_s, moved, *scratch
):
    chunks = len(plan.chunks)
    by_rows, staged, ready = (scratch[k * chunks : (k + 1) * chunks] for k in range(3))
    (
        source, old_owner, new_owner, owner_row, row_counts, all_counts, grad, steps, sizes,
        small_sem, grad_sem, local_sem, sent, recv1, recv2, recv_c,
        row_in, up_in, mate_in, far_up,
    ) = scratch[3 * chunks :]
    olds = (old_m, old_f, old_s)
    groups_x, groups_y, experts, held, rows = plan.groups_x, plan.groups_y, plan.experts, plan.held, plan.rows
    devices = groups_x * groups_y
    splits = groups_x // plan.tiles
    planes = groups_y // PAIR
    half = planes // 2
    gx = lax.axis_index("gx")
    gy = lax.axis_index("gy")
    me = gx * groups_y + gy
    plane = gy // PAIR
    side = gy % PAIR
    mate = gy + 1 - 2 * side
    upper = plane // half
    has_low = plane > 0
    has_high = plane < planes - 1

    core = gx % CORES
    peers_x = [gx]
    for k in range(1, groups_x // CORES):
        peers_x += [(gx - core + CORES * k) % groups_x + CORES - 1 - c for c in range(CORES)]
    peers_x += [gx - core + (core + k) % CORES for k in range(1, CORES)]

    def signal(sem, px, py):
        pl.semaphore_signal(sem, inc=1, device_id=(px, py), device_id_type=MESH)

    barrier = pltpu.get_barrier_semaphore()
    for off in range(1, groups_x):
        signal(barrier, peers_x[off], gy)

    def greet(k):
        signal(barrier, gx, gy + k * PAIR)
        pl.when(side == 0)(lambda: signal(barrier, gx, mate + k * PAIR))

    for k in range(1, planes):
        pl.when(plane + k < planes)(functools.partial(greet, k))

    pl.when(side == 0)(lambda: signal(barrier, gx, mate))

    small = (
        pltpu.make_async_copy(old_owner_hbm, old_owner, small_sem),
        pltpu.make_async_copy(new_owner_hbm, new_owner, small_sem),
        pltpu.make_async_copy(owner_row_hbm, owner_row, small_sem),
        pltpu.make_async_copy(count_row, row_counts.at[gx], small_sem),
    )
    grad_copy = pltpu.make_async_copy(grad_hbm, grad, grad_sem)

    def landed(ref, sem):
        pltpu.make_async_copy(ref, ref, sem).wait()

    def columns(chunk, part):
        start = (part % splits) * plan.span + plan.chunks[chunk].start
        return pl.ds(pl.multiple_of(start, LANES), plan.chunks[chunk].width)

    def tile_base(base, part):
        return pl.multiple_of(base + (part // splits) * SUBLANES, SUBLANES)

    def tile_rows(chunk, base, part):
        return pl.ds(tile_base(base, part) + plan.chunks[chunk].row, plan.chunks[chunk].rows)

    def own_rows(chunk):
        return by_rows[chunk].at[pl.ds(gx * held, held)]

    def load(chunk):
        state = plan.chunks[chunk].state
        for off in [*range(1, groups_x), 0]:
            part = peers_x[off]
            target = own_rows(chunk) if off == 0 else ready[chunk].at[off - 1]
            piece = olds[state].at[:, tile_rows(chunk, 0, part), columns(chunk, part)]
            pltpu.make_async_copy(piece, target, local_sem.at[0 if chunk < FIRST_LOADS else 1]).start()

    def first_sends(chunk):
        for off in range(1, groups_x):
            pltpu.make_async_remote_copy(
                src_ref=ready[chunk].at[off - 1],
                dst_ref=own_rows(chunk),
                send_sem=sent,
                recv_sem=recv1.at[chunk],
                device_id=(peers_x[off], gy),
                device_id_type=MESH,
            ).start()

    def count_copy(rows, k, sem, px, py):
        return pltpu.make_async_remote_copy(
            src_ref=rows.at[k],
            dst_ref=rows.at[k],
            send_sem=sent,
            recv_sem=recv_c.at[sem],
            device_id=(px, py),
            device_id_type=MESH,
        )

    for chunk in range(FIRST_LOADS):
        load(chunk)
    for copy in small:
        copy.start()
    for chunk in range(FIRST_LOADS, chunks):
        load(chunk)
    grad_copy.start()

    pl.semaphore_wait(barrier, groups_x - 1 + plane * (1 + side) + side)
    for off in range(1, groups_x):
        signal(row_in, peers_x[off], gy)

    for chunk in range(FIRST_LOADS):
        landed(by_rows[chunk], local_sem.at[0])
    for chunk in range(FIRST_LOADS):
        first_sends(chunk)
    for copy in small:
        copy.wait()
    for off in range(1, groups_x):
        count_copy(row_counts, gx, 0, peers_x[off], gy).start()
    for chunk in range(FIRST_LOADS, chunks):
        landed(by_rows[chunk], local_sem.at[1])
    for chunk in range(FIRST_LOADS, chunks):
        first_sends(chunk)

    owners = [new_owner[e] for e in range(experts)]
    places = [old_owner[e] for e in range(experts)]

    def find(slot, carry):
        total = jnp.int32(0)
        for e in range(experts):
            total = total + jnp.where(owners[e] == slot, places[e], 0)
        source[slot] = total
        return carry

    pl.semaphore_wait(row_in, groups_x - 1)

    @pl.when(side == 1)
    def _():
        signal(mate_in, gx, mate)

        @pl.when(has_low)
        def _():
            signal(up_in, gx, gy - PAIR)
            signal(up_in, gx, mate - PAIR)

    lax.fori_loop(0, experts, find, 0)

    pl.when(side == 0)(lambda: pl.semaphore_wait(mate_in, 1))

    def meet_upper():
        pl.semaphore_wait(up_in, 1)
        if planes > 2:
            pl.when(has_low)(lambda: signal(far_up.at[0], gx, gy - PAIR))

    pl.when(upper == 0)(meet_upper)

    def landing(chunk):
        return moved.at[plan.chunks[chunk].state, tile_rows(chunk, gy * rows, gx), columns(chunk, gx)]

    def send(chunk, px, py):
        pltpu.make_async_remote_copy(
            src_ref=staged[chunk].at[px * groups_y + py],
            dst_ref=landing(chunk),
            send_sem=sent,
            recv_sem=recv2.at[plan.chunks[chunk].lands],
            device_id=(px, py),
            device_id_type=MESH,
        ).start()

    def send_counts():
        landed(row_counts.at[pl.ds(0, groups_x - 1)], recv_c.at[0])
        all_counts[gy] = jnp.sum(row_counts[...], axis=0)
        for off in range(1, groups_y):
            count_copy(all_counts, gy, 1, gx, (gy + off) % groups_y).start()

    def to_plane(fn, target):
        for pair in range(PAIR):
            py = target * PAIR + (side + pair + 1) % PAIR
            for px in peers_x[1:] + peers_x[:1]:
                fn(px, py)

    def to_own_plane(fn):
        for px in peers_x:
            fn(px, mate)
        for px in peers_x[1:]:
            fn(px, gy)

    def to_upper(fns, far):
        pl.semaphore_wait(far_up.at[far - 2], 1)
        if far < planes - 1:
            pl.when(has_low)(lambda: signal(far_up.at[far - 1], gx, gy - PAIR))
        for fn in fns:
            to_plane(fn, plane + far)

    def spread_last(fn):
        row = CORES
        corner = [(0, px) for px in reversed(range(row))]
        rest = [(pair, px) for pair in range(PAIR) for px in range(groups_x) if (pair, px) not in corner]

        def to_part(target, part):
            for pair, px in part:
                fn(px, target * PAIR + pair)

        def downward():
            for part in (corner, rest):
                for target in range(half):
                    to_part(target, part)

        def upward():
            for part in (corner, rest):
                for target in range(half, planes):
                    to_part(target, part)

        pl.when(upper == 1)(downward)
        pl.when(upper == 0)(upward)
        for k in range(1, half):
            to_plane(fn, upper * half + (plane + k) % half)
        to_own_plane(fn)

    def spread(fn):
        for k in range(half):
            to_plane(fn, upper * k + (1 - upper) * (planes - 1 - k))
        for k in range(1, half):
            to_plane(fn, upper * half + (plane + k) % half)
        to_own_plane(fn)

    def stage(chunk):
        landed(ready[chunk], recv1.at[chunk])

        def one(slot, carry):
            staged[chunk][slot] = by_rows[chunk][source[slot]]
            return carry

        lax.fori_loop(0, experts, one, 0, unroll=4)
        if chunk >= FIRST_LOADS:
            landing(chunk)[...] = by_rows[chunk][source[me]]
        elif chunk == FIRST_LOADS - 1:
            own = [by_rows[k][source[me]] for k in range(FIRST_LOADS)]
            moved[TURNS[0], pl.ds(tile_base(gy * rows, gx), SUBLANES), columns(0, gx)] = jnp.concatenate(own)

    opening = {far: FIRST_LOADS + far - 3 for far in range(2, planes)}
    early = opening[planes - 1] + 1
    for chunk in range(early):
        stage(chunk)
        fn = functools.partial(send, chunk)
        pl.when(upper == 0)(functools.partial(to_plane, fn, plane + 1))
        for k in range(1, planes):
            pl.when(plane >= k)(functools.partial(to_plane, fn, plane - k))
        above = jnp.logical_and(upper == 1, has_high)
        if chunk == 0:
            pl.when(above)(meet_upper)
        pl.when(above)(functools.partial(to_plane, fn, plane + 1))
        for far, opens in opening.items():
            if chunk > opens:
                pl.when(plane < planes - far)(functools.partial(to_plane, fn, plane + far))
            if chunk == opens:
                fns = [functools.partial(send, k) for k in range(chunk + 1)]
                pl.when(plane < planes - far)(functools.partial(to_upper, fns, far))
        to_own_plane(fn)

    def step(chunk):
        stage(chunk)
        (spread_last if chunk == chunks - 1 else spread)(functools.partial(send, chunk))

    for chunk in range(early, chunks):
        step(chunk)
        if chunk == early:
            send_counts()

    landed(all_counts.at[pl.ds(0, groups_y - 1)], recv_c.at[1])
    grad_copy.wait()
    totals = jnp.sum(all_counts[...].astype(jnp.float32), axis=0)
    slot_count = jnp.sum(jnp.where(owner_row[...] == me, totals, 0.0), axis=1, keepdims=True)
    per_token = 1.0 / slot_count

    def tiles(start, width, fn):
        def one(step, carry):
            row = pl.ds(pl.multiple_of(step * ADAM_ROWS, ADAM_ROWS), ADAM_ROWS)
            for part in range(splits):
                fn(row, pl.ds(part * plan.span + start, width))
            return carry

        lax.fori_loop(0, rows * groups_y // ADAM_ROWS, one, 0, unroll=2)

    def moments(row, col):
        moved[FIRST, row, col], moved[SECOND, row, col], steps[row, col] = adam_direction(
            moved[FIRST, row, col], moved[SECOND, row, col], grad[0, row, col], per_token
        )

    def weights(row, col):
        moved[MASTER, row, col] = adam_weights(moved[MASTER, row, col], steps[row, col])

    def all_landed(group, states, width):
        landed(sizes.at[:, :, pl.ds(0, states * width)], recv2.at[group])

    last_start, last_width = plan.bands[-1]
    all_landed(EARLY_BANDS, STATES, last_start)
    for start, width in plan.bands[:-1]:
        tiles(start, width, moments)
        tiles(start, width, weights)
    all_landed(LAST_MOMENTS, STATES - 1, last_width)
    tiles(last_start, last_width, moments)
    all_landed(LAST_WEIGHTS, 1, last_width)
    tiles(last_start, last_width, weights)

    landed(row_counts.at[pl.ds(0, groups_x - 1)], sent)
    landed(all_counts.at[pl.ds(0, groups_y - 1)], sent)
    for chunk in range(chunks):
        landed(ready[chunk], sent)
        landed(staged[chunk].at[pl.ds(0, devices - 1)], sent)


def publish_kernel(moved, master, first, second, sem):
    rows = master.shape[1] // PUBLISHED
    copies = [
        pltpu.make_async_copy(moved.at[pl.ds(k, 1), pl.ds(part * rows, rows)], out.at[:, pl.ds(part * rows, rows)], sem)
        for k, out in enumerate((master, first, second))
        for part in range(PUBLISHED)
    ]
    for copy in copies:
        copy.start()
    for copy in copies:
        copy.wait()


class Chunk(NamedTuple):
    state: int
    start: int
    width: int
    row: int
    rows: int
    lands: int


class Plan:
    def __init__(self, groups_x, groups_y, shape, experts):
        self.groups_x, self.groups_y, self.experts = groups_x, groups_y, experts
        self.held, self.rows, cols = shape
        self.fits = False
        if self.rows % SUBLANES or experts != groups_x * groups_y or groups_x % CORES or groups_y % (2 * PAIR) or groups_y == 2 * PAIR:
            return
        self.tiles = self.rows // SUBLANES
        if groups_x % self.tiles or self.rows * groups_y % ADAM_ROWS:
            return
        self.span = cols // (groups_x // self.tiles)
        if self.span % LANES or cols % (groups_x // self.tiles):
            return
        blocks = self.span // LANES
        widths = [1, *[BAND] * ((blocks - 1) // BAND), (blocks - 1) % BAND]
        widths = WIDTHS if sum(WIDTHS) == blocks else [width for width in widths if width]
        self.bands = [(LANES * sum(widths[:k]), LANES * width) for k, width in enumerate(widths)]
        self.chunks = []
        for start, width in self.bands:
            for state in TURNS:
                lands = EARLY_BANDS
                if (start, width) == self.bands[-1]:
                    lands = LAST_WEIGHTS if state == MASTER else LAST_MOMENTS
                pieces = FIRST_LOADS if not self.chunks else 1
                for k in range(pieces):
                    size = SUBLANES // pieces
                    self.chunks.append(Chunk(state, start, width, k * size, size, lands))
        self.fits = len(widths) > 1 and len(self.chunks) > FIRST_LOADS + groups_y // PAIR


def kernel_body(plan, old_master, old_first, old_second, new_grad, counts, old_owner, new_owner):
    experts = plan.experts
    devices = plan.groups_x * plan.groups_y
    chunks = len(plan.chunks)
    rows, cols = plan.rows * plan.groups_y, old_master.shape[2]
    vmem = pl.BlockSpec(memory_space=pltpu.VMEM)
    hbm = pl.BlockSpec(memory_space=pltpu.HBM)
    far = max(plan.groups_y // PAIR - 2, 1)
    by_rows = [pltpu.VMEM((experts, chunk.rows, chunk.width), jnp.float32) for chunk in plan.chunks]
    ready = [
        pltpu.VMEM((plan.groups_x - 1, plan.held, chunk.rows, chunk.width), jnp.float32) for chunk in plan.chunks
    ]
    row = new_owner.reshape(1, experts)
    operands = (
        old_owner, new_owner, row, counts.reshape(1, experts), new_grad, old_master, old_first, old_second,
    )
    kept = [pltpu.with_memory_space_constraint(array, pltpu.HBM) for array in operands]
    moved = pl.pallas_call(
        functools.partial(rehome_kernel, plan),
        out_shape=jax.ShapeDtypeStruct((STATES, rows, cols), jnp.float32),
        in_specs=[hbm] * 8,
        out_specs=vmem,
        scratch_shapes=by_rows * 2
        + ready
        + [
            pltpu.SMEM((experts,), jnp.int32),
            pltpu.SMEM((experts,), jnp.int32),
            pltpu.SMEM((experts,), jnp.int32),
            pltpu.VMEM((1, experts), jnp.int32),
            pltpu.VMEM((plan.groups_x, 1, experts), jnp.int32),
            pltpu.VMEM((plan.groups_y, 1, experts), jnp.int32),
            pltpu.VMEM((1, rows, cols), new_grad.dtype),
            pltpu.VMEM((rows, cols), jnp.float32),
            pltpu.VMEM((devices - 1, SUBLANES, STATES * plan.span), jnp.float32),
            pltpu.SemaphoreType.DMA,
            pltpu.SemaphoreType.DMA,
            pltpu.SemaphoreType.DMA((2,)),
            pltpu.SemaphoreType.DMA,
            pltpu.SemaphoreType.DMA((chunks,)),
            pltpu.SemaphoreType.DMA((3,)),
            pltpu.SemaphoreType.DMA((2,)),
            pltpu.SemaphoreType.REGULAR,
            pltpu.SemaphoreType.REGULAR,
            pltpu.SemaphoreType.REGULAR,
            pltpu.SemaphoreType.REGULAR((far,)),
        ],
        compiler_params=pltpu.CompilerParams(collective_id=0, has_side_effects=True, vmem_limit_bytes=VMEM_GRANT),
    )(*kept)
    return pl.pallas_call(
        publish_kernel,
        out_shape=[jax.ShapeDtypeStruct((1, rows, cols), jnp.float32)] * STATES,
        in_specs=[pl.BlockSpec(memory_space=pl.ANY)],
        out_specs=[hbm] * STATES,
        scratch_shapes=[pltpu.SemaphoreType.DMA],
        compiler_params=pltpu.CompilerParams(vmem_limit_bytes=1 << 20),
    )(moved)


def body(old_master, old_first, old_second, new_grad, counts, old_owner, new_owner):
    plan = Plan(lax.axis_size("gx"), lax.axis_size("gy"), old_master.shape, old_owner.shape[0])
    if not plan.fits:
        return plain_body(old_master, old_first, old_second, new_grad, counts, old_owner, new_owner)
    return kernel_body(plan, old_master, old_first, old_second, new_grad, counts, old_owner, new_owner)


def solution(mesh):
    placed = (
        P("gx", "gy", None),
        P("gx", "gy", None),
        P("gx", "gy", None),
        P(("gx", "gy"), None, None),
        P(None, ("gx", "gy")),
        P(),
        P(),
    )
    return jax.shard_map(
        body,
        mesh=mesh,
        in_specs=placed,
        out_specs=(P(("gx", "gy"), None, None),) * 3,
        check_vma=False,
    )
```
